32 devices in a mesh: row: 2 (over core), col: 16 (over z, y, x).
Axes of the slice: x: 2, y: 2, z: 4, core: 2. Of those that a mesh axis runs over, the one named last changes fastest.
Arguments:
- object_in: float32 [2, 2, 512, 4096], P(None, None, 'row', 'col'), may hold values from -4 to 4
- probe_in: float32 [2, 256, 256], replicated, may hold values from -5 to 5
- positions: int32 [2, 16, 2, 2], P('row', 'col'), may hold values from -32 to 32
- intensity: float32 [2, 16, 2, 256, 256], P('row', 'col'), may hold values from 0.1 to 8.2
Outputs:
- object_out: float32 [2, 2, 512, 4096], P(None, None, 'row', 'col')
- probe_out: float32 [2, 256, 256], replicated
The draws below stay inside these ranges and needn't reach their ends.
Inputs may be any that keep to these rules, and one draw needn't show every extreme that they name: positions[r, c, p] = (dy, dx) places the probe of position p on object rows r * 256 + dy to r * 256 + dy + 255 and columns c * 256 + dx to c * 256 + dx + 255.
All inputs are finite; a program needn't handle non-finite values.
Results may differ from the reference program's by a relative error of at most 0.0003.
Values sent between devices are 32-bit elements; how exact they have to be, the bound alone decides.
No kernel may reach another device: no remote copies, remote signals or barrier semaphores. Data moves between devices by JAX's collectives and lax.ppermute only.
A program may use at most 64 MiB of HBM per device.

```python
import math
import jax
import jax.numpy as jnp
from jax import lax

PR = 256
CORE = 256
RIM = 32
NPOS = 2
ITERS = 1
TROWS = 2
TCOLS = 16
TILES = 32
NY = 512
NX = 4096


def draw_intensity(key, part):
    shape_all = (TROWS, TCOLS, NPOS, PR, PR)
    tile_number = (jnp.arange(TROWS, dtype=jnp.int32)[:, None] * TCOLS + jnp.arange(TCOLS, dtype=jnp.int32)[None, :]).astype(jnp.float32)
    rising = 1.0 + 2.0 * tile_number / max(TILES - 1, 1)
    base_values = jnp.exp(jax.random.uniform(key, shape_all, jnp.float32, -2.0, 1.0))
    return (base_values * rising[:, :, None, None, None]).astype(jnp.float32)


def touch_ends(entries, stream_key, least, top_value):
    shape = entries.shape
    spot = [jax.random.randint(jax.random.fold_in(stream_key, axis), (), 0, shape[axis]) for axis in range(len(shape))]
    entries = entries.at[tuple(spot)].set(least)
    longest = shape.index(max(shape))
    spot[longest] = (spot[longest] + 1) % shape[longest]
    return entries.at[tuple(spot)].set(top_value)


def shard_levels(stream_key, shape, cuts, least, high):
    def one(axis_at, blocks):
        heights = jax.random.uniform(jax.random.fold_in(jax.random.fold_in(stream_key, 6), axis_at), (blocks,), jnp.float32, least / len(cuts), high / len(cuts))
        return jnp.repeat(jnp.exp(heights), shape[axis_at] // blocks).reshape((-1,) + (1,) * (len(shape) - axis_at - 1))

    factor_of = one(*cuts[0])
    for cut in cuts[1:]:
        factor_of = factor_of * one(*cut)
    return factor_of


def normal_values(stream_key, shape, spread, reach, cuts=(), kind=jnp.bfloat16):
    values = spread * jax.random.normal(stream_key, shape, jnp.float32)
    if cuts:
        values = values * shard_levels(stream_key, shape, cuts, -0.22, 0.18)
    return jnp.clip(values, -reach, reach).astype(kind)


def setup_inputs(seed: int = 0) -> dict:
    arg_keys = jax.random.split(jax.random.key(seed), 5)
    return {
        "object_in": normal_values(arg_keys[0], (2, 2, NY, NX), 0.7, 4.0, ((2, 2), (3, 16)), jnp.float32),
        "probe_in": normal_values(arg_keys[1], (2, PR, PR), 1.0, 5.0, (), jnp.float32),
        "positions": touch_ends(jax.random.randint(arg_keys[2], (TROWS, TCOLS, NPOS, 2), -RIM, RIM + 1), jax.random.fold_in(arg_keys[2], 1), -RIM, RIM).astype(jnp.int32),
        "intensity": draw_intensity(jax.random.fold_in(arg_keys[4], 71), 0),
    }


def tables(extent):
    line_idx = jnp.arange(extent, dtype=jnp.int32)
    turn_count = line_idx[:, None] * line_idx[None, :] % extent
    angles = turn_count.astype(jnp.float32) * (2.0 * math.pi / extent)
    factor = 1.0 / math.sqrt(extent)
    cosine = jnp.cos(angles) * factor
    sine_tab = jnp.sin(angles) * factor
    frequency = ((line_idx + extent // 2) % extent - extent // 2).astype(jnp.float32)
    phases = -math.pi * 8.0 / (extent * extent) * (frequency[:, None] ** 2 + frequency[None, :] ** 2)
    return (cosine, sine_tab, jnp.cos(phases), jnp.sin(phases))

def matrices(cosine, sine_tab, orient):
    return (cosine, sine_tab, float(orient))

def transform(real_part, imag_part, tables_pair):
    cosine, sine_tab, orient = tables_pair
    high = lax.Precision.HIGHEST
    rc = jnp.einsum('byx,xk->byk', real_part, cosine, precision=high)
    rs = jnp.einsum('byx,xk->byk', real_part, sine_tab, precision=high)
    ic = jnp.einsum('byx,xk->byk', imag_part, cosine, precision=high)
    isn = jnp.einsum('byx,xk->byk', imag_part, sine_tab, precision=high)
    mid_re = rc + orient * isn
    mid_im = ic - orient * rs
    out_re = jnp.einsum('ky,byx->bkx', cosine, mid_re, precision=high) + orient * jnp.einsum('ky,byx->bkx', sine_tab, mid_im, precision=high)
    out_im = jnp.einsum('ky,byx->bkx', cosine, mid_im, precision=high) - orient * jnp.einsum('ky,byx->bkx', sine_tab, mid_re, precision=high)
    return (out_re, out_im)

def times_plain(first_re, first_im, second_re, second_im):
    return (first_re * second_re - first_im * second_im, first_re * second_im + first_im * second_re)

def times_conj(first_re, first_im, second_re, second_im):
    return (first_re * second_re + first_im * second_im, first_re * second_im - first_im * second_re)

def tile_gradient(window, probe, offsets, measured, constants):
    cosine, sine_tab, kern_re, kern_im = constants
    forward = matrices(cosine, sine_tab, 1)
    backward = matrices(cosine, sine_tab, -1)
    extent = probe.shape[-1]
    zero_idx = jnp.zeros((), jnp.int32)

    def cut_patch(offset):
        return lax.dynamic_slice(window, (zero_idx, zero_idx, (offset[0] + RIM).astype(jnp.int32), (offset[1] + RIM).astype(jnp.int32)), (2, 2, extent, extent))
    patches = jax.vmap(cut_patch)(offsets)
    first_re, first_im = (patches[:, 0, 0], patches[:, 0, 1])
    second_re, second_im = (patches[:, 1, 0], patches[:, 1, 1])
    probe_re, probe_im = (probe[0], probe[1])
    wave_re, wave_im = times_plain(probe_re, probe_im, first_re, first_im)
    spec_re, spec_im = transform(wave_re, wave_im, forward)
    spec_re, spec_im = times_plain(kern_re, kern_im, spec_re, spec_im)
    prop_re, prop_im = transform(spec_re, spec_im, backward)
    exit_re, exit_im = times_plain(prop_re, prop_im, second_re, second_im)
    far_re, far_im = transform(exit_re, exit_im, forward)
    excess = 2.0 * (far_re * far_re + far_im * far_im - measured)
    back_re, back_im = transform(excess * far_re, excess * far_im, backward)
    grad2_re, grad2_im = times_conj(prop_re, prop_im, back_re, back_im)
    lift_re, lift_im = times_conj(second_re, second_im, back_re, back_im)
    lift_re, lift_im = transform(lift_re, lift_im, forward)
    lift_re, lift_im = times_conj(kern_re, kern_im, lift_re, lift_im)
    enter_re, enter_im = transform(lift_re, lift_im, backward)
    grad1_re, grad1_im = times_conj(probe_re, probe_im, enter_re, enter_im)
    probe_re_g, probe_im_g = times_conj(first_re, first_im, enter_re, enter_im)
    probe_grad = jnp.stack([lax.optimization_barrier(jnp.sum(probe_re_g, 0)), lax.optimization_barrier(jnp.sum(probe_im_g, 0))], 0)
    pieces = jnp.stack([jnp.stack([grad1_re, grad1_im], 1), jnp.stack([grad2_re, grad2_im], 1)], 1)
    gradient = jnp.zeros(window.shape, window.dtype)
    for position in range(offsets.shape[0]):
        start_at = (zero_idx, zero_idx, (offsets[position, 0] + RIM).astype(jnp.int32), (offsets[position, 1] + RIM).astype(jnp.int32))
        current = lax.dynamic_slice(gradient, start_at, pieces.shape[1:])
        gradient = lax.dynamic_update_slice(gradient, current + pieces[position], start_at)
    return (gradient, probe_grad)

def reference(object_in, probe_in, positions, intensity):
    constants = tables(PR)
    current = object_in
    probe = probe_in
    offsets_all = positions.reshape(TILES, NPOS, 2)
    measured_all = intensity.reshape(TILES, NPOS, PR, PR)
    span = CORE + 2 * RIM
    zero_idx = jnp.zeros((), jnp.int32)
    for iteration in range(ITERS):
        padded = jnp.pad(current, ((0, 0), (0, 0), (RIM, RIM), (RIM, RIM)))

        def visit(tile, carry):
            accum, probe_total = carry
            tile_idx = jnp.asarray(tile).astype(jnp.int32)
            row_idx = tile_idx // TCOLS
            col_idx = tile_idx % TCOLS
            start_at = (zero_idx, zero_idx, (row_idx * CORE).astype(jnp.int32), (col_idx * CORE).astype(jnp.int32))
            window = lax.dynamic_slice(padded, start_at, (2, 2, span, span))
            offsets = lax.dynamic_index_in_dim(offsets_all, tile_idx, 0, keepdims=False)
            measured = lax.dynamic_index_in_dim(measured_all, tile_idx, 0, keepdims=False)
            gradient, probe_grad = tile_gradient(window, probe, offsets, measured, constants)
            placed = lax.dynamic_slice(accum, start_at, (2, 2, span, span)) + gradient
            return (lax.dynamic_update_slice(accum, placed, start_at), probe_total + probe_grad.astype(probe_total.dtype))
        accum, probe_total = lax.fori_loop(0, TILES, visit, (jnp.zeros(padded.shape, padded.dtype), jnp.zeros(probe.shape, probe.dtype)))
        descent = accum[:, :, RIM:RIM + NY, RIM:RIM + NX]
        largest = jnp.max(descent[:, 0] ** 2 + descent[:, 1] ** 2)
        current = current - 0.3 * descent / (jnp.sqrt(largest) + 1e-06)
        probe = probe - 2.0 / TILES * probe_total
    return (current, probe)
```

```python
import functools
import math

import jax
import jax.numpy as jnp
import numpy as np
from jax import lax
from jax.experimental import pallas as pl
from jax.experimental.pallas import tpu as pltpu
from jax.sharding import PartitionSpec as P

RIM = 32
LANES = 128
PLANES = 4
VMEM = pl.BlockSpec(memory_space=pltpu.VMEM)
SMEM = pl.BlockSpec(memory_space=pltpu.SMEM)
f32 = jnp.float32
bf16 = jnp.bfloat16


def split_np(table):
    high = table.astype(np.float32).astype(jnp.bfloat16)
    low = (table - high.astype(np.float64)).astype(np.float32).astype(jnp.bfloat16)
    return high, low


def tables(extent):
    line = np.arange(extent)
    angle = (np.outer(line, line) % extent) * (2.0 * math.pi / extent)
    cosine = np.cos(angle) / math.sqrt(extent)
    sine = np.sin(angle) / math.sqrt(extent)
    frequency = (line + extent // 2) % extent - extent // 2
    kernel = np.exp(-1j * math.pi * 8.0 / (extent * extent) * frequency.astype(np.float64) ** 2)
    forward = cosine - 1j * sine
    travel = (np.conj(forward) * kernel[None, :]) @ forward
    parts = []
    for table in (travel.real, travel.imag, cosine, sine):
        parts.extend(split_np(table))
    return np.stack(parts)


def split(value):
    high = value.astype(bf16)
    low = (value - high.astype(f32)).astype(bf16)
    return high, low


def lanes_of(rows):
    return lax.broadcasted_iota(jnp.int32, (rows, LANES), 1)


def pack_kernel(par, obj, col1, col2, *row_msgs):
    extent = obj.shape[-1]
    lane = lanes_of(extent)
    left = jnp.zeros((extent, LANES), f32)
    right = jnp.zeros((extent, LANES), f32)
    for q in range(PLANES):
        inside = (lane >= RIM * q) & (lane < RIM * (q + 1))
        head = obj[q, :, :LANES]
        tail = obj[q, :, extent - LANES :]
        head = pltpu.roll(head, RIM * q, 1) if q else head
        tail = pltpu.roll(tail, (RIM * q + RIM) % LANES, 1) if (RIM * q + RIM) % LANES else tail
        left = jnp.where(inside, head, left)
        right = jnp.where(inside, tail, right)
    odd_col = par[1] == 1
    col1[...] = jnp.where(odd_col, left, right)
    col2[...] = jnp.where(odd_col, right, left)
    for n, msg in enumerate(row_msgs):
        at_top = (par[0] + n) % 2
        start = pl.multiple_of((1 - at_top) * (extent - RIM), RIM)
        for q in range(PLANES):
            msg[RIM * q : RIM * (q + 1), :] = obj[q, pl.ds(start, RIM), :]


def tile_kernel(sides, pos, par, obj, col1, col2, *rest):
    row_in = rest[:sides]
    corner_in = rest[sides : 2 * sides]
    probe, measured, tabs = rest[2 * sides : 2 * sides + 3]
    outs = rest[2 * sides + 3 :]
    row_out = outs[:sides]
    keep_out, inner_out, left_out, right_out = outs[sides : sides + 4]
    window, grad, patch, wave, mats, right_in, left_in = outs[sides + 4 :]
    extent = obj.shape[-1]
    tiles = extent // LANES
    count = pos.shape[0]
    span = extent + 2 * RIM
    lane = lanes_of(extent)
    odd_row = par[0]
    odd_col = par[1] == 1

    for part in range(2):
        a_re, a_im, cosine, sine = (tabs[2 * t + part] for t in range(4))
        for index, diag, upper, lower in (
            (0, a_re, a_im, -a_im),
            (1, a_re, -a_im, a_im),
            (2, cosine, -sine, sine),
            (3, cosine, sine, -sine),
        ):
            mats[index, part, :extent, :extent] = diag
            mats[index, part, extent:, extent:] = diag
            mats[index, part, :extent, extent:] = upper
            mats[index, part, extent:, :extent] = lower

    rim1 = col1[...]
    rim2 = col2[...]
    from_left = jnp.where(odd_col, rim1, rim2)
    from_right = jnp.where(odd_col, rim2, rim1)
    if sides == 1:
        start = pl.multiple_of(odd_row * (extent + RIM), RIM)
        for q in range(PLANES):
            for t in range(tiles + 2):
                window[q, t, pl.ds(start, RIM), :] = jnp.zeros((RIM, LANES), f32)
    starts = [pl.multiple_of((1 - (odd_row + n) % 2) * (extent + RIM), RIM) for n in range(sides)]
    for q in range(PLANES):
        turn_left = (LANES - RIM - RIM * q) % LANES
        turn_right = (LANES - RIM * q) % LANES
        turned = lambda value, turn: pltpu.roll(value, turn, 1) if turn else value
        window[q, 0, RIM : RIM + extent, :] = turned(from_left, turn_left)
        window[q, tiles + 1, RIM : RIM + extent, :] = turned(from_right, turn_right)
        for t in range(tiles):
            window[q, t + 1, RIM : RIM + extent, :] = obj[q, :, LANES * t : LANES * (t + 1)]
        for n in range(sides):
            corner1 = corner_in[n][:RIM, :]
            corner2 = corner_in[n][RIM:, :]
            window[q, 0, pl.ds(starts[n], RIM), :] = turned(jnp.where(odd_col, corner1, corner2), turn_left)
            window[q, tiles + 1, pl.ds(starts[n], RIM), :] = turned(jnp.where(odd_col, corner2, corner1), turn_right)
            for t in range(tiles):
                window[q, t + 1, pl.ds(starts[n], RIM), :] = row_in[n][RIM * q : RIM * (q + 1), LANES * t : LANES * (t + 1)]

    for q in range(PLANES):
        for t in range(tiles + 2):
            grad[q, t] = jnp.zeros((span, LANES), f32)

    def place(p):
        across = pos[p, 1] + LANES
        return pos[p, 0] + RIM, across // LANES, across % LANES

    def cols(c):
        return slice(c * extent, (c + 1) * extent)

    def to_right(p, re, im):
        for c, value in ((0, re), (1, im)):
            high, low = split(value)
            right_in[0, cols(p), cols(c)] = high
            right_in[1, cols(p), cols(c)] = low

    def right_stage(index):
        for p in range(count):
            for c in range(2):
                first = jnp.dot(right_in[0, cols(p), :], mats[index, 0, :, cols(c)], preferred_element_type=f32)
                first += jnp.dot(right_in[0, cols(p), :], mats[index, 1, :, cols(c)], preferred_element_type=f32)
                first += jnp.dot(right_in[1, cols(p), :], mats[index, 0, :, cols(c)], preferred_element_type=f32)
                high, low = split(first)
                left_in[0, cols(c), cols(p)] = high
                left_in[1, cols(c), cols(p)] = low

    def left_stage(index, p):
        out = []
        for c in range(2):
            first = jnp.dot(mats[index, 0, cols(c), :], left_in[0, :, cols(p)], preferred_element_type=f32)
            first += jnp.dot(mats[index, 1, cols(c), :], left_in[0, :, cols(p)], preferred_element_type=f32)
            first += jnp.dot(mats[index, 0, cols(c), :], left_in[1, :, cols(p)], preferred_element_type=f32)
            out.append(first)
        return out

    def add_piece(p, q, value):
        down, first, turn = place(p)
        moved = [pltpu.roll(value[:, LANES * t : LANES * (t + 1)], turn, 1) for t in range(tiles)]
        for t in range(tiles + 1):
            if t == 0:
                piece = jnp.where(lane >= turn, moved[0], 0.0)
            elif t == tiles:
                piece = jnp.where(lane >= turn, 0.0, moved[t - 1])
            else:
                piece = jnp.where(lane >= turn, moved[t], moved[t - 1])
            grad[q, first + t, pl.ds(down, extent), :] += piece

    for p in range(count):
        down, first, turn = place(p)
        back = (LANES - turn) % LANES
        for q in range(PLANES):
            got = [pltpu.roll(window[q, first + t, pl.ds(down, extent), :], back, 1) for t in range(tiles + 1)]
            for t in range(tiles):
                patch[p, q, :, LANES * t : LANES * (t + 1)] = jnp.where(lane < LANES - turn, got[t], got[t + 1])
        pr, pi = probe[0], probe[1]
        ar, ai = patch[p, 0], patch[p, 1]
        to_right(p, pr * ar - pi * ai, pr * ai + pi * ar)
    right_stage(0)
    for p in range(count):
        qr, qi = left_stage(1, p)
        wave[p, 0] = qr
        wave[p, 1] = qi
        br, bi = patch[p, 2], patch[p, 3]
        to_right(p, qr * br - qi * bi, qr * bi + qi * br)
    right_stage(2)
    for p in range(count):
        fr, fi = left_stage(3, p)
        excess = 2.0 * (fr * fr + fi * fi - measured[p])
        to_right(p, excess * fr, excess * fi)
    right_stage(3)
    for p in range(count):
        hr, hi = left_stage(2, p)
        qr, qi = wave[p, 0], wave[p, 1]
        add_piece(p, 2, qr * hr + qi * hi)
        add_piece(p, 3, qr * hi - qi * hr)
        br, bi = patch[p, 2], patch[p, 3]
        to_right(p, br * hr + bi * hi, br * hi - bi * hr)
    right_stage(1)
    total_re = total_im = None
    for p in range(count):
        er, ei = left_stage(0, p)
        pr, pi = probe[0], probe[1]
        add_piece(p, 0, pr * er + pi * ei)
        add_piece(p, 1, pr * ei - pi * er)
        ar, ai = patch[p, 0], patch[p, 1]
        gr = ar * er + ai * ei
        gi = ar * ei - ai * er
        if p:
            gr = wave[0, 0] + gr
            gi = wave[0, 1] + gi
        wave[0, 0] = gr
        wave[0, 1] = gi
    is_odd = odd_row == 1
    keep_out[...] = jnp.where(is_odd, wave[0, 1], wave[0, 0])
    row_out[0][:extent, :] = jnp.where(is_odd, wave[0, 0], wave[0, 1])

    def packed(tile, left, start, rows):
        out = jnp.zeros((rows, LANES), f32)
        narrow = lanes_of(rows)
        for q in range(PLANES):
            value = grad[q, tile, pl.ds(start, rows), :]
            turn = (RIM * q + (RIM if left else 0)) % LANES
            value = pltpu.roll(value, turn, 1) if turn else value
            out = jnp.where((narrow >= RIM * q) & (narrow < RIM * (q + 1)), value, out)
        return out

    left_out[...] = packed(0, True, RIM, extent)
    right_out[...] = packed(tiles + 1, False, RIM, extent)
    for q in range(PLANES):
        for t in range(tiles):
            inner_out[q, :, LANES * t : LANES * (t + 1)] = grad[q, t + 1, RIM : RIM + extent, :]
    for n in range(sides):
        base = extent if n == 0 else 0
        for q in range(PLANES):
            for t in range(tiles):
                row_out[n][base + RIM * q : base + RIM * (q + 1), LANES * t : LANES * (t + 1)] = grad[q, t + 1, pl.ds(starts[n], RIM), :]
        at = base + RIM * PLANES
        row_out[n][at : at + RIM, :LANES] = packed(0, True, starts[n], RIM)
        row_out[n][at : at + RIM, LANES : 2 * LANES] = packed(tiles + 1, False, starts[n], RIM)


def cols_kernel(sides, par, keep, left, right, *rest):
    row_in = rest[:sides]
    msg1, msg2, keep2, edge = rest[sides:]
    extent = left.shape[0]
    half = extent // 2
    odd_col = par[1] == 1
    for n in range(sides):
        base = (extent if n == 0 else 0) + RIM * PLANES
        start = pl.multiple_of((1 - (par[0] + n) % 2) * (extent - RIM), RIM)
        if n == 0:
            edge[0] = left[...]
            edge[1] = right[...]
        for s in range(2):
            edge[s, pl.ds(start, RIM), :] += row_in[n][base : base + RIM, LANES * s : LANES * (s + 1)]
    to1 = jnp.where(odd_col, edge[0], edge[1])
    to2 = jnp.where(odd_col, edge[1], edge[0])
    lower = keep[:half, :] + row_in[0][:half, :]
    upper = keep[half:, :] + row_in[0][half:extent, :]
    keep2[...] = jnp.where(odd_col, upper, lower)
    msg1[:half, :] = jnp.where(odd_col, lower, upper)
    msg1[half:, :LANES] = to1[:half]
    msg1[half:, LANES:] = to1[half:]
    msg2[:, :LANES] = to2[:half]
    msg2[:, LANES:] = to2[half:]


def gather_kernel(sides, par, inner, keep3, got3, col1, col2, *rest):
    row_in = rest[:sides]
    msg, descent = rest[sides:]
    extent = inner.shape[-1]
    half = extent // 2
    quarter = keep3.shape[0]
    tiles = extent // LANES
    odd_col = par[1] == 1
    lane = lanes_of(half)
    descent[...] = inner[...]
    for n in range(sides):
        base = extent if n == 0 else 0
        start = pl.multiple_of((1 - (par[0] + n) % 2) * (extent - RIM), RIM)
        for q in range(PLANES):
            descent[q, pl.ds(start, RIM), :] += row_in[n][base + RIM * q : base + RIM * (q + 1), :]
    for s in range(2):
        rim1 = col1[half:, LANES * s : LANES * (s + 1)]
        rim2 = col2[:, LANES * s : LANES * (s + 1)]
        from_left = jnp.where(odd_col, rim1, rim2)
        from_right = jnp.where(odd_col, rim2, rim1)
        rows = slice(half * s, half * (s + 1))
        for q in range(PLANES):
            turn_left = (LANES - RIM * q) % LANES
            turn_right = (LANES - RIM - RIM * q) % LANES
            on_left = pltpu.roll(from_left, turn_left, 1) if turn_left else from_left
            on_right = pltpu.roll(from_right, turn_right, 1) if turn_right else from_right
            descent[q, rows, :LANES] += jnp.where(lane < RIM, on_left, 0.0)
            descent[q, rows, extent - LANES :] += jnp.where(lane >= LANES - RIM, on_right, 0.0)
    peak = None
    for s in range(2):
        power = descent[2 * s] * descent[2 * s] + descent[2 * s + 1] * descent[2 * s + 1]
        power = jnp.max(power.reshape(extent // 8, 8, extent), axis=0)
        peak = power if peak is None else jnp.maximum(peak, power)
    msg[:quarter, :] = keep3[...] + got3[...]
    msg[quarter:, :] = peak


def final_kernel(rate, par, obj, descent, probe, mine, other, obj_out, probe_out):
    extent = obj.shape[-1]
    odd_row = par[0] == 1
    peak = jnp.max(jnp.maximum(mine[extent:, :], other[extent:, :]))
    peak = jnp.broadcast_to(peak, (8, extent))
    scale = (0.3 / (jnp.sqrt(peak) + 1e-06))[:1, :]
    for q in range(PLANES):
        obj_out[q] = obj[q] - descent[q] * scale
    probe_out[0] = probe[0] - rate * jnp.where(odd_row, other[:extent, :], mine[:extent, :])
    probe_out[1] = probe[1] - rate * jnp.where(odd_row, mine[:extent, :], other[:extent, :])


def call(kernel, outs, ins, scratch=(), smem=1, name=None):
    return pl.pallas_call(
        kernel,
        out_shape=tuple(jax.ShapeDtypeStruct(shape, f32) for shape in outs),
        in_specs=[SMEM] * smem + [VMEM] * (len(ins) - smem),
        out_specs=tuple(VMEM for _ in outs),
        scratch_shapes=list(scratch),
        compiler_params=pltpu.CompilerParams(vmem_limit_bytes=48 * 1024 * 1024),
        name=name,
    )(*ins)


def swap(value, axis, bit):
    count = lax.axis_size(axis)
    return lax.ppermute(value, axis, [(i, i ^ bit) for i in range(count)])


def pairs(value, axis, phase):
    count = lax.axis_size(axis)
    links = []
    for i in range(phase, count - 1, 2):
        links += [(i, i + 1), (i + 1, i)]
    return lax.ppermute(value, axis, links)


def local(object_in, probe_in, positions, intensity):
    extent = probe_in.shape[-1]
    half, quarter = extent // 2, extent // 4
    rows, cols = lax.axis_size("row"), lax.axis_size("col")
    sides = 1 if rows == 2 else 2
    row, col = lax.axis_index("row"), lax.axis_index("col")
    par = jnp.stack([row % 2, col % 2]).astype(jnp.int32)
    offsets = positions.reshape(-1, 2)
    count = offsets.shape[0]
    measured = intensity.reshape(-1, extent, extent)
    obj = object_in.reshape(PLANES, extent, extent)
    tabs = jnp.asarray(tables(extent))

    sent = call(pack_kernel, [(extent, LANES)] * 2 + [(PLANES * RIM, extent)] * sides, (par, obj), name="pack")
    col2 = pairs(sent[1], "col", 1)
    col1 = pairs(sent[0], "col", 0)
    row_in = [pairs(sent[2 + n], "row", n) for n in range(sides)]
    corner_in = []
    for n in range(sides):
        start = jnp.where((row + n) % 2 == 0, extent - RIM, 0)
        corner = jnp.concatenate([lax.dynamic_slice_in_dim(c, start, RIM, 0) for c in (col1, col2)], 0)
        corner_in.append(pairs(corner, "row", n))

    span = extent + 2 * RIM
    tiles = extent // LANES
    rim_rows = RIM * (PLANES + 1)
    wide = (2 * extent, 2 * extent)
    out = call(
        functools.partial(tile_kernel, sides),
        [(extent + rim_rows, extent)] + [(rim_rows, extent)] * (sides - 1)
        + [(extent, extent), (PLANES, extent, extent), (extent, LANES), (extent, LANES)],
        (offsets, par, obj, col1, col2, *row_in, *corner_in, probe_in, measured, tabs),
        scratch=[
            pltpu.VMEM((PLANES, tiles + 2, span, LANES), f32),
            pltpu.VMEM((PLANES, tiles + 2, span, LANES), f32),
            pltpu.VMEM((count, PLANES, extent, extent), f32),
            pltpu.VMEM((count, 2, extent, extent), f32),
            pltpu.VMEM((4, 2) + wide, bf16),
            pltpu.VMEM((2, count * extent, 2 * extent), bf16),
            pltpu.VMEM((2, 2 * extent, count * extent), bf16),
        ],
        smem=2,
        name="tile",
    )
    row_back = [pairs(out[n], "row", n) for n in range(sides)]
    keep, inner, left, right = out[sides:]
    msg1, msg2, keep2 = call(
        functools.partial(cols_kernel, sides),
        [(extent, extent), (half, extent), (half, extent)],
        (par, keep, left, right, *row_back),
        scratch=[pltpu.VMEM((2, extent, LANES), f32)],
        name="cols",
    )
    got1 = pairs(msg1, "col", 0)
    got2 = pairs(msg2, "col", 1)
    both = keep2 + got1[:half]
    up = (col // 2) % 2 == 1
    keep3 = jnp.where(up, both[quarter:], both[:quarter])
    got3 = swap(jnp.where(up, both[:quarter], both[quarter:]), "col", 2)
    state, descent = call(
        functools.partial(gather_kernel, sides),
        [(quarter + 8, extent), (PLANES, extent, extent)],
        (par, inner, keep3, got3, got1, got2, *row_back),
        name="gather",
    )
    is_sum = lax.broadcasted_iota(jnp.int32, state.shape, 0) < quarter
    steps = [("col", 1 << b) for b in range(2, cols.bit_length() - 1)]
    steps += [("row", 1 << b) for b in range(1, rows.bit_length() - 1)]
    for axis, bit in steps:
        other = swap(state, axis, bit)
        state = jnp.where(is_sum, state + other, jnp.maximum(state, other))

    def joined(state, other, up):
        top = state.shape[0] - 8
        low = jnp.where(up, other[:top], state[:top])
        high = jnp.where(up, state[:top], other[:top])
        return jnp.concatenate([low, high, jnp.maximum(state[top:], other[top:])], 0)

    state = joined(state, swap(state, "col", 2), up)
    state = joined(state, swap(state, "col", 1), col % 2 == 1)
    other = swap(state, "row", 1)
    object_out, probe_out = call(
        functools.partial(final_kernel, 2.0 / (rows * cols)),
        [obj.shape, probe_in.shape],
        (par, obj, descent, probe_in, state, other),
        name="final",
    )
    return object_out.reshape(object_in.shape), probe_out


def solution(mesh):
    placed = (
        P(None, None, "row", "col"),
        P(),
        P("row", "col", None, None),
        P("row", "col", None, None, None),
    )
    return jax.shard_map(
        local,
        mesh=mesh,
        in_specs=placed,
        out_specs=(P(None, None, "row", "col"), P()),
        check_vma=False,
    )
```

```python
import functools
import math

import jax
import jax.numpy as jnp
import numpy as np
from jax import lax
from jax.experimental import pallas as pl
from jax.experimental.pallas import tpu as pltpu
from jax.sharding import PartitionSpec as P


RIM = 32
LANES = 128
PLANES = 4
VMEM = pl.BlockSpec(memory_space=pltpu.VMEM)
SMEM = pl.BlockSpec(memory_space=pltpu.SMEM)
HBM = pl.BlockSpec(memory_space=pltpu.HBM)
f32 = jnp.float32
bf16 = jnp.bfloat16


def split_np(table):
    high = table.astype(np.float32).astype(jnp.bfloat16)
    low = (table - high.astype(np.float64)).astype(np.float32).astype(jnp.bfloat16)
    return high, low


def tables(extent):
    line = np.arange(extent)
    angle = (np.outer(line, line) % extent) * (2.0 * math.pi / extent)
    cosine = np.cos(angle) / math.sqrt(extent)
    sine = np.sin(angle) / math.sqrt(extent)
    frequency = (line + extent // 2) % extent - extent // 2
    kernel = np.exp(-1j * math.pi * 8.0 / (extent * extent) * frequency.astype(np.float64) ** 2)
    forward = cosine - 1j * sine
    travel = (np.conj(forward) * kernel[None, :]) @ forward
    parts = []
    for table in (travel.real, travel.imag, cosine, sine):
        parts.extend(split_np(table))
    return np.stack(parts)


def split(value):
    high = value.astype(bf16)
    low = (value - high.astype(f32)).astype(bf16)
    return high, low


def lanes_of(rows):
    return lax.broadcasted_iota(jnp.int32, (rows, LANES), 1)


def pack_kernel(par, obj_hbm, obj, col1, col2, *rest):
    row_msgs, sem = rest[:-1], rest[-1]
    extent = obj.shape[-1]
    lane = lanes_of(extent)
    left = jnp.zeros((extent, LANES), f32)
    right = jnp.zeros((extent, LANES), f32)
    copies = [pltpu.make_async_copy(obj_hbm.at[q], obj.at[q], sem.at[q]) for q in range(PLANES)]
    for copy in copies:
        copy.start()
    for q in range(PLANES):
        copies[q].wait()
        inside = (lane >= RIM * q) & (lane < RIM * (q + 1))
        head = obj[q, :, :LANES]
        tail = obj[q, :, extent - LANES :]
        head = pltpu.roll(head, RIM * q, 1) if q else head
        tail = pltpu.roll(tail, (RIM * q + RIM) % LANES, 1) if (RIM * q + RIM) % LANES else tail
        left = jnp.where(inside, head, left)
        right = jnp.where(inside, tail, right)
    odd_col = par[1] == 1
    col1[...] = jnp.where(odd_col, left, right)
    col2[...] = jnp.where(odd_col, right, left)
    for n, msg in enumerate(row_msgs):
        at_top = (par[0] + n) % 2
        start = pl.multiple_of((1 - at_top) * (extent - RIM), RIM)
        for q in range(PLANES):
            msg[RIM * q : RIM * (q + 1), :] = obj[q, pl.ds(start, RIM), :]


def prep_kernel(par, obj, probe_hbm, measured_hbm, tabs_hbm, probe, measured, mats, window, mask2, mask4, tabs, sem):
    extent = obj.shape[-1]
    tiles = extent // LANES
    copies = [
        pltpu.make_async_copy(tabs_hbm, tabs, sem.at[0]),
        pltpu.make_async_copy(probe_hbm, probe, sem.at[1]),
        pltpu.make_async_copy(measured_hbm, measured, sem.at[2]),
    ]
    for copy in copies:
        copy.start()
    for q in range(PLANES):
        for t in range(tiles + 2):
            window[q, t, :RIM, :] = jnp.zeros((RIM, LANES), f32)
            window[q, t, RIM + extent :, :] = jnp.zeros((RIM, LANES), f32)
        for t in range(tiles):
            window[q, t + 1, RIM : RIM + extent, :] = obj[q, :, LANES * t : LANES * (t + 1)]
    mask2[...] = jnp.full(mask2.shape, par[2], jnp.int32).astype(f32)
    mask4[...] = jnp.full(mask4.shape, par[3], jnp.int32).astype(f32)
    copies[0].wait()
    for part in range(2):
        a_re, a_im, cosine, sine = (tabs[2 * t + part] for t in range(4))
        for index, diag, upper, lower in (
            (0, a_re, a_im, -a_im),
            (1, a_re, -a_im, a_im),
            (2, cosine, -sine, sine),
            (3, cosine, sine, -sine),
        ):
            mats[index, part, :extent, :extent] = diag
            mats[index, part, extent:, extent:] = diag
            mats[index, part, :extent, extent:] = upper
            mats[index, part, extent:, :extent] = lower
    copies[1].wait()
    copies[2].wait()


def tile_kernel(sides, pos, par, col1, col2, *rest):
    row_in = rest[:sides]
    corner_in = rest[sides : 2 * sides]
    probe, measured, mats, _ = rest[2 * sides : 2 * sides + 4]
    outs = rest[2 * sides + 4 :]
    row_out = outs[:sides]
    keep_out, inner_out, left_out, right_out, window = outs[sides : sides + 5]
    grad, patch, wave, right_in, left_in = outs[sides + 5 :]
    extent = probe.shape[-1]
    tiles = extent // LANES
    count = pos.shape[0]
    span = extent + 2 * RIM
    lane = lanes_of(extent)
    odd_row = par[0]
    odd_col = par[1] == 1

    rim1 = col1[...]
    rim2 = col2[...]
    from_left = jnp.where(odd_col, rim1, rim2)
    from_right = jnp.where(odd_col, rim2, rim1)
    starts = [pl.multiple_of((1 - (odd_row + n) % 2) * (extent + RIM), RIM) for n in range(sides)]
    for q in range(PLANES):
        turn_left = (LANES - RIM - RIM * q) % LANES
        turn_right = (LANES - RIM * q) % LANES
        turned = lambda value, turn: pltpu.roll(value, turn, 1) if turn else value
        window[q, 0, RIM : RIM + extent, :] = turned(from_left, turn_left)
        window[q, tiles + 1, RIM : RIM + extent, :] = turned(from_right, turn_right)
        for n in range(sides):
            corner1 = corner_in[n][:RIM, :]
            corner2 = corner_in[n][RIM:, :]
            window[q, 0, pl.ds(starts[n], RIM), :] = turned(jnp.where(odd_col, corner1, corner2), turn_left)
            window[q, tiles + 1, pl.ds(starts[n], RIM), :] = turned(jnp.where(odd_col, corner2, corner1), turn_right)
            for t in range(tiles):
                window[q, t + 1, pl.ds(starts[n], RIM), :] = row_in[n][RIM * q : RIM * (q + 1), LANES * t : LANES * (t + 1)]

    for q in range(PLANES):
        for t in range(tiles + 2):
            grad[q, t] = jnp.zeros((span, LANES), f32)

    def place(p):
        across = pos[p, 1] + LANES
        return pos[p, 0] + RIM, across // LANES, across % LANES

    def cols(c):
        return slice(c * extent, (c + 1) * extent)

    def to_right(p, re, im):
        for c, value in ((0, re), (1, im)):
            high, low = split(value)
            right_in[0, cols(p), cols(c)] = high
            right_in[1, cols(p), cols(c)] = low

    def right_stage(index):
        for p in range(count):
            for c in range(2):
                first = jnp.dot(right_in[0, cols(p), :], mats[index, 0, :, cols(c)], preferred_element_type=f32)
                first += jnp.dot(right_in[0, cols(p), :], mats[index, 1, :, cols(c)], preferred_element_type=f32)
                first += jnp.dot(right_in[1, cols(p), :], mats[index, 0, :, cols(c)], preferred_element_type=f32)
                high, low = split(first)
                left_in[0, cols(c), cols(p)] = high
                left_in[1, cols(c), cols(p)] = low

    def left_stage(index, p):
        out = []
        for c in range(2):
            first = jnp.dot(mats[index, 0, cols(c), :], left_in[0, :, cols(p)], preferred_element_type=f32)
            first += jnp.dot(mats[index, 1, cols(c), :], left_in[0, :, cols(p)], preferred_element_type=f32)
            first += jnp.dot(mats[index, 0, cols(c), :], left_in[1, :, cols(p)], preferred_element_type=f32)
            out.append(first)
        return out

    def add_piece(p, q, value):
        down, first, turn = place(p)
        moved = [pltpu.roll(value[:, LANES * t : LANES * (t + 1)], turn, 1) for t in range(tiles)]
        for t in range(tiles + 1):
            if t == 0:
                piece = jnp.where(lane >= turn, moved[0], 0.0)
            elif t == tiles:
                piece = jnp.where(lane >= turn, 0.0, moved[t - 1])
            else:
                piece = jnp.where(lane >= turn, moved[t], moved[t - 1])
            grad[q, first + t, pl.ds(down, extent), :] += piece

    for p in range(count):
        down, first, turn = place(p)
        back = (LANES - turn) % LANES
        for q in range(PLANES):
            got = [pltpu.roll(window[q, first + t, pl.ds(down, extent), :], back, 1) for t in range(tiles + 1)]
            for t in range(tiles):
                patch[p, q, :, LANES * t : LANES * (t + 1)] = jnp.where(lane < LANES - turn, got[t], got[t + 1])
        pr, pi = probe[0], probe[1]
        ar, ai = patch[p, 0], patch[p, 1]
        to_right(p, pr * ar - pi * ai, pr * ai + pi * ar)
    right_stage(0)
    for p in range(count):
        qr, qi = left_stage(1, p)
        wave[p, 0] = qr
        wave[p, 1] = qi
        br, bi = patch[p, 2], patch[p, 3]
        to_right(p, qr * br - qi * bi, qr * bi + qi * br)
    right_stage(2)
    for p in range(count):
        fr, fi = left_stage(3, p)
        excess = 2.0 * (fr * fr + fi * fi - measured[p])
        to_right(p, excess * fr, excess * fi)
    right_stage(3)
    for p in range(count):
        hr, hi = left_stage(2, p)
        qr, qi = wave[p, 0], wave[p, 1]
        add_piece(p, 2, qr * hr + qi * hi)
        add_piece(p, 3, qr * hi - qi * hr)
        br, bi = patch[p, 2], patch[p, 3]
        to_right(p, br * hr + bi * hi, br * hi - bi * hr)
    right_stage(1)
    for p in range(count):
        er, ei = left_stage(0, p)
        pr, pi = probe[0], probe[1]
        add_piece(p, 0, pr * er + pi * ei)
        add_piece(p, 1, pr * ei - pi * er)
        ar, ai = patch[p, 0], patch[p, 1]
        gr = ar * er + ai * ei
        gi = ar * ei - ai * er
        if p:
            gr = wave[0, 0] + gr
            gi = wave[0, 1] + gi
        wave[0, 0] = gr
        wave[0, 1] = gi
    is_odd = odd_row == 1
    keep_out[...] = jnp.where(is_odd, wave[0, 1], wave[0, 0])
    row_out[0][:extent, :] = jnp.where(is_odd, wave[0, 0], wave[0, 1])

    def packed(tile, left, start, rows):
        out = jnp.zeros((rows, LANES), f32)
        narrow = lanes_of(rows)
        for q in range(PLANES):
            value = grad[q, tile, pl.ds(start, rows), :]
            turn = (RIM * q + (RIM if left else 0)) % LANES
            value = pltpu.roll(value, turn, 1) if turn else value
            out = jnp.where((narrow >= RIM * q) & (narrow < RIM * (q + 1)), value, out)
        return out

    left_out[...] = packed(0, True, RIM, extent)
    right_out[...] = packed(tiles + 1, False, RIM, extent)
    for q in range(PLANES):
        for t in range(tiles):
            inner_out[q, :, LANES * t : LANES * (t + 1)] = grad[q, t + 1, RIM : RIM + extent, :]
    for n in range(sides):
        base = extent if n == 0 else 0
        for q in range(PLANES):
            for t in range(tiles):
                row_out[n][base + RIM * q : base + RIM * (q + 1), LANES * t : LANES * (t + 1)] = grad[q, t + 1, pl.ds(starts[n], RIM), :]
        at = base + RIM * PLANES
        row_out[n][at : at + RIM, :LANES] = packed(0, True, starts[n], RIM)
        row_out[n][at : at + RIM, LANES : 2 * LANES] = packed(tiles + 1, False, starts[n], RIM)


def corner_kernel(par, col1, col2, *msgs):
    extent = col1.shape[0]
    for n, msg in enumerate(msgs):
        start = pl.multiple_of((1 - (par[0] + n) % 2) * (extent - RIM), RIM)
        msg[:RIM, :] = col1[pl.ds(start, RIM), :]
        msg[RIM:, :] = col2[pl.ds(start, RIM), :]


def split_kernel(par, mine, other, keep, send):
    half = mine.shape[0] // 2
    kept = pl.multiple_of(par[3] * half, half)
    sent = pl.multiple_of((1 - par[3]) * half, half)
    keep[...] = mine[pl.ds(kept, half), :] + other[pl.ds(kept, half), :]
    send[...] = mine[pl.ds(sent, half), :] + other[pl.ds(sent, half), :]


def cols_kernel(sides, par, keep, left, right, *rest):
    row_in = rest[:sides]
    probe_msg, probe_keep, msg1, msg2, edge = rest[sides:]
    extent = left.shape[0]
    half = extent // 2
    odd_col = par[1] == 1
    up = par[2] == 1
    edge[0] = left[...]
    edge[1] = right[...]
    for n in range(sides):
        base = (extent if n == 0 else 0) + RIM * PLANES
        start = pl.multiple_of((1 - (par[0] + n) % 2) * (extent - RIM), RIM)
        for s in range(2):
            edge[s, pl.ds(start, RIM), :] += row_in[n][base : base + RIM, LANES * s : LANES * (s + 1)]
    to1 = jnp.where(odd_col, edge[0], edge[1])
    to2 = jnp.where(odd_col, edge[1], edge[0])
    lower = keep[:half, :] + row_in[0][:half, :]
    upper = keep[half:, :] + row_in[0][half:extent, :]
    probe_keep[...] = jnp.where(up, upper, lower)
    probe_msg[...] = jnp.where(up, lower, upper)
    for msg, value in ((msg1, to1), (msg2, to2)):
        msg[:, :LANES] = value[:half]
        msg[:, LANES:] = value[half:]


def gather_kernel(sides, par, inner, keep3, got3, col1, col2, *rest):
    row_in = rest[:sides]
    msg, descent = rest[sides:]
    extent = inner.shape[-1]
    half = extent // 2
    quarter = keep3.shape[0]
    odd_col = par[1] == 1
    lane = lanes_of(half)
    descent[...] = inner[...]
    for n in range(sides):
        base = extent if n == 0 else 0
        start = pl.multiple_of((1 - (par[0] + n) % 2) * (extent - RIM), RIM)
        for q in range(PLANES):
            descent[q, pl.ds(start, RIM), :] += row_in[n][base + RIM * q : base + RIM * (q + 1), :]
    for s in range(2):
        rim1 = col1[:, LANES * s : LANES * (s + 1)]
        rim2 = col2[:, LANES * s : LANES * (s + 1)]
        from_left = jnp.where(odd_col, rim1, rim2)
        from_right = jnp.where(odd_col, rim2, rim1)
        rows = slice(half * s, half * (s + 1))
        for q in range(PLANES):
            turn_left = (LANES - RIM * q) % LANES
            turn_right = (LANES - RIM - RIM * q) % LANES
            on_left = pltpu.roll(from_left, turn_left, 1) if turn_left else from_left
            on_right = pltpu.roll(from_right, turn_right, 1) if turn_right else from_right
            descent[q, rows, :LANES] += jnp.where(lane < RIM, on_left, 0.0)
            descent[q, rows, extent - LANES :] += jnp.where(lane >= LANES - RIM, on_right, 0.0)
    peak = None
    for s in range(2):
        power = descent[2 * s] * descent[2 * s] + descent[2 * s + 1] * descent[2 * s + 1]
        power = jnp.max(power.reshape(extent // 8, 8, extent), axis=0)
        peak = power if peak is None else jnp.maximum(peak, power)
    msg[:quarter, :] = keep3[...] + got3[...]
    msg[quarter:, :] = peak


def final_kernel(rate, par, obj, descent, probe, mine, other, obj_out, probe_out, buf, sem):
    extent = obj.shape[-1]
    odd_row = par[0] == 1
    sums = (jnp.where(odd_row, other[:extent, :], mine[:extent, :]), jnp.where(odd_row, mine[:extent, :], other[:extent, :]))
    copies = [pltpu.make_async_copy(buf.at[q], obj_out.at[q], sem.at[q]) for q in range(PLANES)]
    copies += [pltpu.make_async_copy(buf.at[PLANES + c], probe_out.at[c], sem.at[PLANES + c]) for c in range(2)]
    for c in range(2):
        buf[PLANES + c] = probe[c] - rate * sums[c]
        copies[PLANES + c].start()
    peak = jnp.max(jnp.maximum(mine[extent:, :], other[extent:, :]))
    peak = jnp.broadcast_to(peak, (8, extent))
    scale = (0.3 / (jnp.sqrt(peak) + 1e-06))[:1, :]
    for q in range(PLANES):
        buf[q] = obj[q] - descent[q] * scale
        copies[q].start()
    for copy in copies:
        copy.wait()


def call(kernel, outs, ins, scratch=(), smem=1, in_hbm=(), out_hbm=(), alias=None, limit=8):
    shapes = [out if isinstance(out, jax.ShapeDtypeStruct) else jax.ShapeDtypeStruct(out, f32) for out in outs]
    return pl.pallas_call(
        kernel,
        out_shape=tuple(shapes),
        in_specs=[SMEM if i < smem else HBM if i in in_hbm else VMEM for i in range(len(ins))],
        out_specs=tuple(HBM if i in out_hbm else VMEM for i in range(len(outs))),
        scratch_shapes=list(scratch),
        input_output_aliases=alias or {},
        compiler_params=pltpu.CompilerParams(vmem_limit_bytes=limit * 1024 * 1024),
    )(*[pltpu.with_memory_space_constraint(x, pltpu.HBM) if i in in_hbm else x for i, x in enumerate(ins)])


def swap(value, axis, bit):
    count = lax.axis_size(axis)
    return lax.ppermute(value, axis, [(i, i ^ bit) for i in range(count)])


def pairs(value, axis, phase):
    count = lax.axis_size(axis)
    links = []
    for i in range(phase, count - 1, 2):
        links += [(i, i + 1), (i + 1, i)]
    return lax.ppermute(value, axis, links)


def step(object_in, probe_in, positions, intensity):
    extent = probe_in.shape[-1]
    half, quarter = extent // 2, extent // 4
    rows, cols = lax.axis_size("row"), lax.axis_size("col")
    sides = 1 if rows == 2 else 2
    row, col = lax.axis_index("row"), lax.axis_index("col")
    par = jnp.stack([row & 1, col & 1, (col >> 1) & 1, (col >> 2) & 1]).astype(jnp.int32)
    offsets = positions.reshape(-1, 2)
    count = offsets.shape[0]
    measured_in = intensity.reshape(-1, extent, extent)
    obj_in = object_in.reshape(PLANES, extent, extent)
    tabs = jnp.asarray(tables(extent))
    span = extent + 2 * RIM
    tiles = extent // LANES
    rim_rows = RIM * (PLANES + 1)

    obj, *sent = call(
        pack_kernel,
        [obj_in.shape] + [(extent, LANES)] * 2 + [(PLANES * RIM, extent)] * sides,
        (par, obj_in),
        scratch=[pltpu.SemaphoreType.DMA((PLANES,))],
        in_hbm=(1,),
    )
    col2 = pairs(sent[1], "col", 1)
    col1 = pairs(sent[0], "col", 0)
    row_in = [pairs(sent[2 + n], "row", n) for n in range(sides)]
    probe, measured, mats, window, mask2, mask4 = call(
        prep_kernel,
        [
            probe_in.shape,
            measured_in.shape,
            jax.ShapeDtypeStruct((4, 2, 2 * extent, 2 * extent), bf16),
            (PLANES, tiles + 2, span, LANES),
            (half, extent),
            (quarter, extent),
        ],
        (par, obj, probe_in, measured_in, tabs),
        scratch=[pltpu.VMEM(tabs.shape, bf16), pltpu.SemaphoreType.DMA((3,))],
        in_hbm=(2, 3, 4),
        limit=16,
    )
    corners = call(corner_kernel, [(2 * RIM, LANES)] * sides, (par, col1, col2))
    corner_in = [pairs(corners[n], "row", n) for n in range(sides)]

    ins = (offsets, par, col1, col2, *row_in, *corner_in, probe, measured, mats, window)
    shapes = [(extent + rim_rows, extent)] + [(rim_rows, extent)] * (sides - 1)
    shapes += [(extent, extent), (PLANES, extent, extent), (extent, LANES), (extent, LANES), window.shape]
    out = call(
        functools.partial(tile_kernel, sides),
        shapes,
        ins,
        scratch=[
            pltpu.VMEM((PLANES, tiles + 2, span, LANES), f32),
            pltpu.VMEM((count, PLANES, extent, extent), f32),
            pltpu.VMEM((count, 2, extent, extent), f32),
            pltpu.VMEM((2, count * extent, 2 * extent), bf16),
            pltpu.VMEM((2, 2 * extent, count * extent), bf16),
        ],
        smem=2,
        alias={len(ins) - 1: len(shapes) - 1},
        limit=32,
    )
    row_back = [pairs(out[n], "row", n) for n in range(sides)]
    keep, inner, left, right = out[sides : sides + 4]
    probe_msg, probe_keep, msg1, msg2 = call(
        functools.partial(cols_kernel, sides),
        [(half, extent)] * 4,
        (par, keep, left, right, *row_back),
        scratch=[pltpu.VMEM((2, extent, LANES), f32)],
    )
    probe_got = swap(probe_msg, "col", 2)
    got2 = pairs(msg2, "col", 1)
    got1 = pairs(msg1, "col", 0)
    keep3, send3 = call(split_kernel, [(quarter, extent)] * 2, (par, probe_keep, probe_got))
    got3 = swap(send3, "col", 4)
    state, descent = call(
        functools.partial(gather_kernel, sides),
        [(quarter + 8, extent), (PLANES, extent, extent)],
        (par, inner, keep3, got3, got1, got2, *row_back),
    )
    is_sum = lax.broadcasted_iota(jnp.int32, state.shape, 0) < quarter
    steps = [("col", 1 << b) for b in range(3, cols.bit_length() - 1)] + [("col", 1)]
    steps += [("row", 1 << b) for b in range(1, rows.bit_length() - 1)]
    for axis, bit in steps:
        other = swap(state, axis, bit)
        state = jnp.where(is_sum, state + other, jnp.maximum(state, other))

    def joined(state, other, mask):
        top = state.shape[0] - 8
        up = mask > 0.5
        low = jnp.where(up, other[:top], state[:top])
        high = jnp.where(up, state[:top], other[:top])
        return jnp.concatenate([low, high, jnp.maximum(state[top:], other[top:])], 0)

    state = joined(state, swap(state, "col", 4), mask4)
    state = joined(state, swap(state, "col", 2), mask2)
    other = swap(state, "row", 1)
    object_out, probe_out = call(
        functools.partial(final_kernel, 2.0 / (rows * cols)),
        [obj.shape, probe_in.shape],
        (par, obj, descent, probe, state, other),
        scratch=[pltpu.VMEM((PLANES + 2, extent, extent), f32), pltpu.SemaphoreType.DMA((PLANES + 2,))],
        out_hbm=(0, 1),
    )
    return object_out.reshape(object_in.shape), probe_out


def solution(mesh):
    placed = (
        P(None, None, "row", "col"),
        P(),
        P("row", "col", None, None),
        P("row", "col", None, None, None),
    )
    return jax.shard_map(
        step,
        mesh=mesh,
        in_specs=placed,
        out_specs=(P(None, None, "row", "col"), P()),
        check_vma=False,
    )
```

```python
import functools
import math

import jax
import jax.numpy as jnp
import numpy as np
from jax import lax
from jax.experimental import pallas as pl
from jax.experimental.pallas import tpu as pltpu
from jax.sharding import PartitionSpec as P


RIM = 32
LANES = 128
PLANES = 4
VMEM = pl.BlockSpec(memory_space=pltpu.VMEM)
HBM = pl.BlockSpec(memory_space=pltpu.HBM)
f32 = jnp.float32
bf16 = jnp.bfloat16


def split_np(table):
    high = table.astype(np.float32).astype(jnp.bfloat16)
    low = (table - high.astype(np.float64)).astype(np.float32).astype(jnp.bfloat16)
    return high, low


def tables(extent):
    line = np.arange(extent)
    angle = (np.outer(line, line) % extent) * (2.0 * math.pi / extent)
    cosine = np.cos(angle) / math.sqrt(extent)
    sine = np.sin(angle) / math.sqrt(extent)
    frequency = (line + extent // 2) % extent - extent // 2
    kernel = np.exp(-1j * math.pi * 8.0 / (extent * extent) * frequency.astype(np.float64) ** 2)
    forward = cosine - 1j * sine
    travel = (np.conj(forward) * kernel[None, :]) @ forward
    parts = []
    for table in (travel.real, travel.imag, cosine, sine):
        parts.extend(split_np(table))
    return np.stack(parts)


def split(value):
    high = value.astype(bf16)
    low = (value - high.astype(f32)).astype(bf16)
    return high, low


def lanes_of(rows):
    return lax.broadcasted_iota(jnp.int32, (rows, LANES), 1)


def parities():
    row, col = lax.axis_index("row"), lax.axis_index("col")
    return row & 1, col & 1, (col >> 1) & 1, (col >> 2) & 1


def pack_kernel(obj_hbm, obj, col1, col2, *rest):
    row_msgs, sem = rest[:-1], rest[-1]
    par = parities()
    extent = obj.shape[-1]
    lane = lanes_of(extent)
    left = jnp.zeros((extent, LANES), f32)
    right = jnp.zeros((extent, LANES), f32)
    copies = [pltpu.make_async_copy(obj_hbm.at[q], obj.at[q], sem.at[q]) for q in range(PLANES)]
    for copy in copies:
        copy.start()
    for q in range(PLANES):
        copies[q].wait()
        inside = (lane >= RIM * q) & (lane < RIM * (q + 1))
        head = obj[q, :, :LANES]
        tail = obj[q, :, extent - LANES :]
        head = pltpu.roll(head, RIM * q, 1) if q else head
        tail = pltpu.roll(tail, (RIM * q + RIM) % LANES, 1) if (RIM * q + RIM) % LANES else tail
        left = jnp.where(inside, head, left)
        right = jnp.where(inside, tail, right)
    odd_col = par[1] == 1
    col1[...] = jnp.where(odd_col, left, right)
    col2[...] = jnp.where(odd_col, right, left)
    for n, msg in enumerate(row_msgs):
        at_top = (par[0] + n) % 2
        start = pl.multiple_of((1 - at_top) * (extent - RIM), RIM)
        for q in range(PLANES):
            msg[RIM * q : RIM * (q + 1), :] = obj[q, pl.ds(start, RIM), :]


def prep_kernel(obj, probe_hbm, measured_hbm, tabs_hbm, probe, measured, mats, window, grad, mask2, mask4, tabs, sem):
    extent = obj.shape[-1]
    tiles = extent // LANES
    par = parities()
    copies = [
        pltpu.make_async_copy(tabs_hbm, tabs, sem.at[0]),
        pltpu.make_async_copy(probe_hbm, probe, sem.at[1]),
        pltpu.make_async_copy(measured_hbm, measured, sem.at[2]),
    ]
    for copy in copies:
        copy.start()
    for q in range(PLANES):
        for t in range(tiles + 2):
            grad[q, t] = jnp.zeros(grad.shape[2:], f32)
            window[q, t, :RIM, :] = jnp.zeros((RIM, LANES), f32)
            window[q, t, RIM + extent :, :] = jnp.zeros((RIM, LANES), f32)
        for t in range(tiles):
            window[q, t + 1, RIM : RIM + extent, :] = obj[q, :, LANES * t : LANES * (t + 1)]
    mask2[...] = jnp.full(mask2.shape, par[2], jnp.int32).astype(f32)
    mask4[...] = jnp.full(mask4.shape, par[3], jnp.int32).astype(f32)
    copies[0].wait()
    for part in range(2):
        a_re, a_im, cosine, sine = (tabs[2 * t + part] for t in range(4))
        for index, diag, upper, lower in (
            (0, a_re, a_im, -a_im),
            (1, a_re, -a_im, a_im),
            (2, cosine, -sine, sine),
            (3, cosine, sine, -sine),
        ):
            mats[index, part, :extent, :extent] = diag
            mats[index, part, extent:, extent:] = diag
            mats[index, part, :extent, extent:] = upper
            mats[index, part, extent:, :extent] = lower
    copies[1].wait()
    copies[2].wait()


def tile_kernel(sides, pos_hbm, col1, col2, *rest):
    row_in = rest[:sides]
    corner_in = rest[sides : 2 * sides]
    probe, measured, mats = rest[2 * sides : 2 * sides + 3]
    outs = rest[2 * sides + 5 :]
    row_out = outs[:sides]
    keep_out, inner_out, left_out, right_out, window, grad = outs[sides : sides + 6]
    patch, wave, right_in, left_in, pos, sem = outs[sides + 6 :]
    fetch = pltpu.make_async_copy(pos_hbm, pos, sem)
    fetch.start()
    par = parities()
    extent = probe.shape[-1]
    tiles = extent // LANES
    count = pos.shape[0]
    lane = lanes_of(extent)
    odd_row = par[0]
    odd_col = par[1] == 1

    rim1 = col1[...]
    rim2 = col2[...]
    from_left = jnp.where(odd_col, rim1, rim2)
    from_right = jnp.where(odd_col, rim2, rim1)
    starts = [pl.multiple_of((1 - (odd_row + n) % 2) * (extent + RIM), RIM) for n in range(sides)]
    for q in range(PLANES):
        turn_left = (LANES - RIM - RIM * q) % LANES
        turn_right = (LANES - RIM * q) % LANES
        turned = lambda value, turn: pltpu.roll(value, turn, 1) if turn else value
        window[q, 0, RIM : RIM + extent, :] = turned(from_left, turn_left)
        window[q, tiles + 1, RIM : RIM + extent, :] = turned(from_right, turn_right)
        for n in range(sides):
            corner1 = corner_in[n][:RIM, :]
            corner2 = corner_in[n][RIM:, :]
            window[q, 0, pl.ds(starts[n], RIM), :] = turned(jnp.where(odd_col, corner1, corner2), turn_left)
            window[q, tiles + 1, pl.ds(starts[n], RIM), :] = turned(jnp.where(odd_col, corner2, corner1), turn_right)
            for t in range(tiles):
                window[q, t + 1, pl.ds(starts[n], RIM), :] = row_in[n][RIM * q : RIM * (q + 1), LANES * t : LANES * (t + 1)]

    fetch.wait()

    def place(p):
        across = pos[p, 1] + LANES
        return pos[p, 0] + RIM, across // LANES, across % LANES

    def cols(c):
        return slice(c * extent, (c + 1) * extent)

    def to_right(p, re, im):
        for c, value in ((0, re), (1, im)):
            high, low = split(value)
            right_in[0, cols(p), cols(c)] = high
            right_in[1, cols(p), cols(c)] = low

    def right_stage(index):
        for c in range(2):
            both = jnp.dot(right_in[0], mats[index, 0, :, cols(c)], preferred_element_type=f32)
            both += jnp.dot(right_in[0], mats[index, 1, :, cols(c)], preferred_element_type=f32)
            both += jnp.dot(right_in[1], mats[index, 0, :, cols(c)], preferred_element_type=f32)
            for p in range(count):
                high, low = split(both[cols(p)])
                left_in[0, cols(c), cols(p)] = high
                left_in[1, cols(c), cols(p)] = low

    def left_stage(index, p):
        both = jnp.dot(mats[index, 0], left_in[0, :, cols(p)], preferred_element_type=f32)
        both += jnp.dot(mats[index, 1], left_in[0, :, cols(p)], preferred_element_type=f32)
        both += jnp.dot(mats[index, 0], left_in[1, :, cols(p)], preferred_element_type=f32)
        return both[:extent], both[extent:]

    def add_piece(p, q, value):
        down, first, turn = place(p)
        moved = [pltpu.roll(value[:, LANES * t : LANES * (t + 1)], turn, 1) for t in range(tiles)]
        for t in range(tiles + 1):
            if t == 0:
                piece = jnp.where(lane >= turn, moved[0], 0.0)
            elif t == tiles:
                piece = jnp.where(lane >= turn, 0.0, moved[t - 1])
            else:
                piece = jnp.where(lane >= turn, moved[t], moved[t - 1])
            grad[q, first + t, pl.ds(down, extent), :] += piece

    for p in range(count):
        down, first, turn = place(p)
        back = (LANES - turn) % LANES
        for q in range(PLANES):
            got = [pltpu.roll(window[q, first + t, pl.ds(down, extent), :], back, 1) for t in range(tiles + 1)]
            for t in range(tiles):
                patch[p, q, :, LANES * t : LANES * (t + 1)] = jnp.where(lane < LANES - turn, got[t], got[t + 1])
        pr, pi = probe[0], probe[1]
        ar, ai = patch[p, 0], patch[p, 1]
        to_right(p, pr * ar - pi * ai, pr * ai + pi * ar)
    right_stage(0)
    for p in range(count):
        qr, qi = left_stage(1, p)
        wave[p, 0] = qr
        wave[p, 1] = qi
        br, bi = patch[p, 2], patch[p, 3]
        to_right(p, qr * br - qi * bi, qr * bi + qi * br)
    right_stage(2)
    for p in range(count):
        fr, fi = left_stage(3, p)
        excess = 2.0 * (fr * fr + fi * fi - measured[p])
        to_right(p, excess * fr, excess * fi)
    right_stage(3)
    for p in range(count):
        hr, hi = left_stage(2, p)
        qr, qi = wave[p, 0], wave[p, 1]
        add_piece(p, 2, qr * hr + qi * hi)
        add_piece(p, 3, qr * hi - qi * hr)
        br, bi = patch[p, 2], patch[p, 3]
        to_right(p, br * hr + bi * hi, br * hi - bi * hr)
    right_stage(1)
    for p in range(count):
        er, ei = left_stage(0, p)
        pr, pi = probe[0], probe[1]
        add_piece(p, 0, pr * er + pi * ei)
        add_piece(p, 1, pr * ei - pi * er)
        ar, ai = patch[p, 0], patch[p, 1]
        gr = ar * er + ai * ei
        gi = ar * ei - ai * er
        if p:
            gr = wave[0, 0] + gr
            gi = wave[0, 1] + gi
        wave[0, 0] = gr
        wave[0, 1] = gi
    is_odd = odd_row == 1
    keep_out[...] = jnp.where(is_odd, wave[0, 1], wave[0, 0])
    row_out[0][:extent, :] = jnp.where(is_odd, wave[0, 0], wave[0, 1])

    def packed(tile, left, start, rows):
        out = jnp.zeros((rows, LANES), f32)
        narrow = lanes_of(rows)
        for q in range(PLANES):
            value = grad[q, tile, pl.ds(start, rows), :]
            turn = (RIM * q + (RIM if left else 0)) % LANES
            value = pltpu.roll(value, turn, 1) if turn else value
            out = jnp.where((narrow >= RIM * q) & (narrow < RIM * (q + 1)), value, out)
        return out

    left_out[...] = packed(0, True, RIM, extent)
    right_out[...] = packed(tiles + 1, False, RIM, extent)
    for q in range(PLANES):
        for t in range(tiles):
            inner_out[q, :, LANES * t : LANES * (t + 1)] = grad[q, t + 1, RIM : RIM + extent, :]
    for n in range(sides):
        base = extent if n == 0 else 0
        for q in range(PLANES):
            for t in range(tiles):
                row_out[n][base + RIM * q : base + RIM * (q + 1), LANES * t : LANES * (t + 1)] = grad[q, t + 1, pl.ds(starts[n], RIM), :]
        at = base + RIM * PLANES
        row_out[n][at : at + RIM, :LANES] = packed(0, True, starts[n], RIM)
        row_out[n][at : at + RIM, LANES : 2 * LANES] = packed(tiles + 1, False, starts[n], RIM)


def corner_kernel(col1, col2, *msgs):
    par = parities()
    extent = col1.shape[0]
    for n, msg in enumerate(msgs):
        start = pl.multiple_of((1 - (par[0] + n) % 2) * (extent - RIM), RIM)
        msg[:RIM, :] = col1[pl.ds(start, RIM), :]
        msg[RIM:, :] = col2[pl.ds(start, RIM), :]


def split_kernel(mine, other, keep, send):
    par = parities()
    half = mine.shape[0] // 2
    kept = pl.multiple_of(par[3] * half, half)
    sent = pl.multiple_of((1 - par[3]) * half, half)
    keep[...] = mine[pl.ds(kept, half), :] + other[pl.ds(kept, half), :]
    send[...] = mine[pl.ds(sent, half), :] + other[pl.ds(sent, half), :]


def cols_kernel(sides, keep, left, right, *rest):
    par = parities()
    row_in = rest[:sides]
    probe_msg, probe_keep, msg1, msg2, edge = rest[sides:]
    extent = left.shape[0]
    half = extent // 2
    odd_col = par[1] == 1
    up = par[2] == 1
    edge[0] = left[...]
    edge[1] = right[...]
    for n in range(sides):
        base = (extent if n == 0 else 0) + RIM * PLANES
        start = pl.multiple_of((1 - (par[0] + n) % 2) * (extent - RIM), RIM)
        for s in range(2):
            edge[s, pl.ds(start, RIM), :] += row_in[n][base : base + RIM, LANES * s : LANES * (s + 1)]
    to1 = jnp.where(odd_col, edge[0], edge[1])
    to2 = jnp.where(odd_col, edge[1], edge[0])
    lower = keep[:half, :] + row_in[0][:half, :]
    upper = keep[half:, :] + row_in[0][half:extent, :]
    probe_keep[...] = jnp.where(up, upper, lower)
    probe_msg[...] = jnp.where(up, lower, upper)
    for msg, value in ((msg1, to1), (msg2, to2)):
        msg[:, :LANES] = value[:half]
        msg[:, LANES:] = value[half:]


def gather_kernel(sides, inner, keep3, got3, col1, col2, *rest):
    row_in = rest[:sides]
    msg, descent = rest[sides:]
    par = parities()
    extent = inner.shape[-1]
    half = extent // 2
    quarter = keep3.shape[0]
    odd_col = par[1] == 1
    lane = lanes_of(half)
    descent[...] = inner[...]
    for n in range(sides):
        base = extent if n == 0 else 0
        start = pl.multiple_of((1 - (par[0] + n) % 2) * (extent - RIM), RIM)
        for q in range(PLANES):
            descent[q, pl.ds(start, RIM), :] += row_in[n][base + RIM * q : base + RIM * (q + 1), :]
    for s in range(2):
        rim1 = col1[:, LANES * s : LANES * (s + 1)]
        rim2 = col2[:, LANES * s : LANES * (s + 1)]
        from_left = jnp.where(odd_col, rim1, rim2)
        from_right = jnp.where(odd_col, rim2, rim1)
        rows = slice(half * s, half * (s + 1))
        for q in range(PLANES):
            turn_left = (LANES - RIM * q) % LANES
            turn_right = (LANES - RIM - RIM * q) % LANES
            on_left = pltpu.roll(from_left, turn_left, 1) if turn_left else from_left
            on_right = pltpu.roll(from_right, turn_right, 1) if turn_right else from_right
            descent[q, rows, :LANES] += jnp.where(lane < RIM, on_left, 0.0)
            descent[q, rows, extent - LANES :] += jnp.where(lane >= LANES - RIM, on_right, 0.0)
    peak = None
    for s in range(2):
        power = descent[2 * s] * descent[2 * s] + descent[2 * s + 1] * descent[2 * s + 1]
        power = jnp.max(power.reshape(extent // 8, 8, extent), axis=0)
        peak = power if peak is None else jnp.maximum(peak, power)
    msg[:quarter, :] = keep3[...] + got3[...]
    msg[quarter:, :] = peak


def final_kernel(rate, obj, descent, probe, mine, other, obj_out, probe_out, buf, sem):
    extent = obj.shape[-1]
    odd_row = parities()[0] == 1
    sums = (jnp.where(odd_row, other[:extent, :], mine[:extent, :]), jnp.where(odd_row, mine[:extent, :], other[:extent, :]))
    copies = [pltpu.make_async_copy(buf.at[q], obj_out.at[q], sem.at[q]) for q in range(PLANES)]
    copies += [pltpu.make_async_copy(buf.at[PLANES + c], probe_out.at[c], sem.at[PLANES + c]) for c in range(2)]
    for c in range(2):
        buf[PLANES + c] = probe[c] - rate * sums[c]
        copies[PLANES + c].start()
    peak = jnp.max(jnp.maximum(mine[extent:, :], other[extent:, :]))
    peak = jnp.broadcast_to(peak, (8, extent))
    scale = (0.3 / (jnp.sqrt(peak) + 1e-06))[:1, :]
    for q in range(PLANES):
        buf[q] = obj[q] - descent[q] * scale
        copies[q].start()
    for copy in copies:
        copy.wait()


def call(kernel, outs, ins, scratch=(), in_hbm=(), out_hbm=(), alias=None, limit=8):
    shapes = [out if isinstance(out, jax.ShapeDtypeStruct) else jax.ShapeDtypeStruct(out, f32) for out in outs]
    return pl.pallas_call(
        kernel,
        out_shape=tuple(shapes),
        in_specs=[HBM if i in in_hbm else VMEM for i in range(len(ins))],
        out_specs=tuple(HBM if i in out_hbm else VMEM for i in range(len(outs))),
        scratch_shapes=list(scratch),
        input_output_aliases=alias or {},
        compiler_params=pltpu.CompilerParams(vmem_limit_bytes=limit * 1024 * 1024),
    )(*[pltpu.with_memory_space_constraint(x, pltpu.HBM) if i in in_hbm else x for i, x in enumerate(ins)])


def swap(value, axis, bit):
    count = lax.axis_size(axis)
    return lax.ppermute(value, axis, [(i, i ^ bit) for i in range(count)])


def pairs(value, axis, phase):
    count = lax.axis_size(axis)
    links = []
    for i in range(phase, count - 1, 2):
        links += [(i, i + 1), (i + 1, i)]
    return lax.ppermute(value, axis, links)


def step(object_in, probe_in, positions, intensity):
    extent = probe_in.shape[-1]
    half, quarter = extent // 2, extent // 4
    rows, cols = lax.axis_size("row"), lax.axis_size("col")
    sides = 1 if rows == 2 else 2
    offsets = positions.reshape(-1, 2)
    count = offsets.shape[0]
    measured_in = intensity.reshape(-1, extent, extent)
    obj_in = object_in.reshape(PLANES, extent, extent)
    tabs = jnp.asarray(tables(extent))
    span = extent + 2 * RIM
    tiles = extent // LANES
    rim_rows = RIM * (PLANES + 1)

    obj, *sent = call(
        pack_kernel,
        [obj_in.shape] + [(extent, LANES)] * 2 + [(PLANES * RIM, extent)] * sides,
        (obj_in,),
        scratch=[pltpu.SemaphoreType.DMA((PLANES,))],
        in_hbm=(0,),
    )
    col2 = pairs(sent[1], "col", 1)
    col1 = pairs(sent[0], "col", 0)
    row_in = [pairs(sent[2 + n], "row", n) for n in range(sides)]
    probe, measured, mats, window, grad, mask2, mask4 = call(
        prep_kernel,
        [
            probe_in.shape,
            measured_in.shape,
            jax.ShapeDtypeStruct((4, 2, 2 * extent, 2 * extent), bf16),
            (PLANES, tiles + 2, span, LANES),
            (PLANES, tiles + 2, span, LANES),
            (half, extent),
            (quarter, extent),
        ],
        (obj, probe_in, measured_in, tabs),
        scratch=[pltpu.VMEM(tabs.shape, bf16), pltpu.SemaphoreType.DMA((3,))],
        in_hbm=(1, 2, 3),
        limit=16,
    )
    corners = call(corner_kernel, [(2 * RIM, LANES)] * sides, (col1, col2))
    corner_in = [pairs(corners[n], "row", n) for n in range(sides)]

    ins = (offsets, col1, col2, *row_in, *corner_in, probe, measured, mats, window, grad)
    shapes = [(extent + rim_rows, extent)] + [(rim_rows, extent)] * (sides - 1)
    shapes += [(extent, extent), (PLANES, extent, extent), (extent, LANES), (extent, LANES), window.shape, grad.shape]
    out = call(
        functools.partial(tile_kernel, sides),
        shapes,
        ins,
        scratch=[
            pltpu.VMEM((count, PLANES, extent, extent), f32),
            pltpu.VMEM((count, 2, extent, extent), f32),
            pltpu.VMEM((2, count * extent, 2 * extent), bf16),
            pltpu.VMEM((2, 2 * extent, count * extent), bf16),
            pltpu.SMEM(offsets.shape, jnp.int32),
            pltpu.SemaphoreType.DMA,
        ],
        in_hbm=(0,),
        alias={len(ins) - 2: len(shapes) - 2, len(ins) - 1: len(shapes) - 1},
        limit=32,
    )
    row_back = [pairs(out[n], "row", n) for n in range(sides)]
    keep, inner, left, right = out[sides : sides + 4]
    probe_msg, probe_keep, msg1, msg2 = call(
        functools.partial(cols_kernel, sides),
        [(half, extent)] * 4,
        (keep, left, right, *row_back),
        scratch=[pltpu.VMEM((2, extent, LANES), f32)],
    )
    probe_got = swap(probe_msg, "col", 2)
    got2 = pairs(msg2, "col", 1)
    got1 = pairs(msg1, "col", 0)
    keep3, send3 = call(split_kernel, [(quarter, extent)] * 2, (probe_keep, probe_got))
    got3 = swap(send3, "col", 4)
    state, descent = call(
        functools.partial(gather_kernel, sides),
        [(quarter + 8, extent), (PLANES, extent, extent)],
        (inner, keep3, got3, got1, got2, *row_back),
    )
    is_sum = lax.broadcasted_iota(jnp.int32, state.shape, 0) < quarter
    steps = [("col", 1 << b) for b in range(3, cols.bit_length() - 1)] + [("col", 1)]
    steps += [("row", 1 << b) for b in range(1, rows.bit_length() - 1)]
    for axis, bit in steps:
        other = swap(state, axis, bit)
        state = jnp.where(is_sum, state + other, jnp.maximum(state, other))

    def joined(state, other, mask):
        top = state.shape[0] - 8
        up = mask > 0.5
        low = jnp.where(up, other[:top], state[:top])
        high = jnp.where(up, state[:top], other[:top])
        return jnp.concatenate([low, high, jnp.maximum(state[top:], other[top:])], 0)

    state = joined(state, swap(state, "col", 4), mask4)
    state = joined(state, swap(state, "col", 2), mask2)
    other = swap(state, "row", 1)
    object_out, probe_out = call(
        functools.partial(final_kernel, 2.0 / (rows * cols)),
        [obj.shape, probe_in.shape],
        (obj, descent, probe, state, other),
        scratch=[pltpu.VMEM((PLANES + 2, extent, extent), f32), pltpu.SemaphoreType.DMA((PLANES + 2,))],
        out_hbm=(0, 1),
    )
    return object_out.reshape(object_in.shape), probe_out


def solution(mesh):
    placed = (
        P(None, None, "row", "col"),
        P(),
        P("row", "col", None, None),
        P("row", "col", None, None, None),
    )
    return jax.shard_map(
        step,
        mesh=mesh,
        in_specs=placed,
        out_specs=(P(None, None, "row", "col"), P()),
        check_vma=False,
    )
```

```python
import functools
import math

import jax
import jax.numpy as jnp
import numpy as np
from jax import lax
from jax.experimental import pallas as pl
from jax.experimental.pallas import tpu as pltpu
from jax.sharding import PartitionSpec as P


RIM = 32
LANES = 128
PLANES = 4
VMEM = pl.BlockSpec(memory_space=pltpu.VMEM)
HBM = pl.BlockSpec(memory_space=pltpu.HBM)
f32 = jnp.float32
bf16 = jnp.bfloat16


def split_np(table):
    high = table.astype(np.float32).astype(jnp.bfloat16)
    low = (table - high.astype(np.float64)).astype(np.float32).astype(jnp.bfloat16)
    return high, low


def tables(extent):
    line = np.arange(extent)
    angle = (np.outer(line, line) % extent) * (2.0 * math.pi / extent)
    cosine = np.cos(angle) / math.sqrt(extent)
    sine = np.sin(angle) / math.sqrt(extent)
    frequency = (line + extent // 2) % extent - extent // 2
    kernel = np.exp(-1j * math.pi * 8.0 / (extent * extent) * frequency.astype(np.float64) ** 2)
    forward = cosine - 1j * sine
    travel = (np.conj(forward) * kernel[None, :]) @ forward
    parts = []
    for table in (travel.real, travel.imag, cosine, sine):
        parts.extend(split_np(table))
    return np.stack(parts)


def split(value):
    high = value.astype(bf16)
    low = (value - high.astype(f32)).astype(bf16)
    return high, low


def lanes_of(rows):
    return lax.broadcasted_iota(jnp.int32, (rows, LANES), 1)


def parities():
    row, col = lax.axis_index("row"), lax.axis_index("col")
    return row & 1, col & 1, (col >> 1) & 1, (col >> 2) & 1


def pack_kernel(obj_hbm, obj, col1, col2, *rest):
    row_msgs, sem = rest[:-1], rest[-1]
    par = parities()
    extent = obj.shape[-1]
    lane = lanes_of(extent)
    left = jnp.zeros((extent, LANES), f32)
    right = jnp.zeros((extent, LANES), f32)
    copies = [pltpu.make_async_copy(obj_hbm.at[q], obj.at[q], sem.at[q]) for q in range(PLANES)]
    for copy in copies:
        copy.start()
    for q in range(PLANES):
        copies[q].wait()
        inside = (lane >= RIM * q) & (lane < RIM * (q + 1))
        head = obj[q, :, :LANES]
        tail = obj[q, :, extent - LANES :]
        head = pltpu.roll(head, RIM * q, 1) if q else head
        tail = pltpu.roll(tail, (RIM * q + RIM) % LANES, 1) if (RIM * q + RIM) % LANES else tail
        left = jnp.where(inside, head, left)
        right = jnp.where(inside, tail, right)
    odd_col = par[1] == 1
    col1[...] = jnp.where(odd_col, left, right)
    col2[...] = jnp.where(odd_col, right, left)
    for n, msg in enumerate(row_msgs):
        at_top = (par[0] + n) % 2
        start = pl.multiple_of((1 - at_top) * (extent - RIM), RIM)
        for q in range(PLANES):
            msg[RIM * q : RIM * (q + 1), :] = obj[q, pl.ds(start, RIM), :]


def prep_kernel(obj, probe_hbm, measured_hbm, tabs_hbm, pos_hbm, probe, measured, mats, window, grad, mask2, mask4, pos, tabs, sem):
    extent = obj.shape[-1]
    tiles = extent // LANES
    par = parities()
    copies = [
        pltpu.make_async_copy(tabs_hbm, tabs, sem.at[0]),
        pltpu.make_async_copy(probe_hbm, probe, sem.at[1]),
        pltpu.make_async_copy(measured_hbm, measured, sem.at[2]),
        pltpu.make_async_copy(pos_hbm, pos, sem.at[3]),
    ]
    for copy in copies:
        copy.start()
    for q in range(PLANES):
        for t in range(tiles + 2):
            grad[q, t] = jnp.zeros(grad.shape[2:], f32)
            window[q, t, :RIM, :] = jnp.zeros((RIM, LANES), f32)
            window[q, t, RIM + extent :, :] = jnp.zeros((RIM, LANES), f32)
        for t in range(tiles):
            window[q, t + 1, RIM : RIM + extent, :] = obj[q, :, LANES * t : LANES * (t + 1)]
    mask2[...] = jnp.full(mask2.shape, par[2], jnp.int32).astype(f32)
    mask4[...] = jnp.full(mask4.shape, par[3], jnp.int32).astype(f32)
    copies[0].wait()
    for part in range(2):
        a_re, a_im, cosine, sine = (tabs[2 * t + part] for t in range(4))
        for index, diag, upper, lower in (
            (0, a_re, a_im, -a_im),
            (1, a_re, -a_im, a_im),
            (2, cosine, -sine, sine),
            (3, cosine, sine, -sine),
        ):
            mats[index, part, :extent, :extent] = diag
            mats[index, part, extent:, extent:] = diag
            mats[index, part, :extent, extent:] = upper
            mats[index, part, extent:, :extent] = lower
    for copy in copies[1:]:
        copy.wait()


def tile_kernel(sides, pos_in, col1, col2, *rest):
    row_in = rest[:sides]
    corner_in = rest[sides : 2 * sides]
    probe, measured, mats = rest[2 * sides : 2 * sides + 3]
    outs = rest[2 * sides + 5 :]
    row_out = outs[:sides]
    keep_out, inner_out, left_out, right_out, window, grad = outs[sides : sides + 6]
    patch, wave, right_in, left_in, pos, sem = outs[sides + 6 :]
    fetch = pltpu.make_async_copy(pos_in, pos, sem)
    fetch.start()
    par = parities()
    extent = probe.shape[-1]
    tiles = extent // LANES
    count = pos.shape[0]
    lane = lanes_of(extent)
    odd_row = par[0]
    odd_col = par[1] == 1

    rim1 = col1[...]
    rim2 = col2[...]
    from_left = jnp.where(odd_col, rim1, rim2)
    from_right = jnp.where(odd_col, rim2, rim1)
    starts = [pl.multiple_of((1 - (odd_row + n) % 2) * (extent + RIM), RIM) for n in range(sides)]
    for q in range(PLANES):
        turn_left = (LANES - RIM - RIM * q) % LANES
        turn_right = (LANES - RIM * q) % LANES
        turned = lambda value, turn: pltpu.roll(value, turn, 1) if turn else value
        window[q, 0, RIM : RIM + extent, :] = turned(from_left, turn_left)
        window[q, tiles + 1, RIM : RIM + extent, :] = turned(from_right, turn_right)
        for n in range(sides):
            corner1 = corner_in[n][:RIM, :]
            corner2 = corner_in[n][RIM:, :]
            window[q, 0, pl.ds(starts[n], RIM), :] = turned(jnp.where(odd_col, corner1, corner2), turn_left)
            window[q, tiles + 1, pl.ds(starts[n], RIM), :] = turned(jnp.where(odd_col, corner2, corner1), turn_right)
            for t in range(tiles):
                window[q, t + 1, pl.ds(starts[n], RIM), :] = row_in[n][RIM * q : RIM * (q + 1), LANES * t : LANES * (t + 1)]

    fetch.wait()

    def place(p):
        across = pos[p, 1] + LANES
        return pos[p, 0] + RIM, across // LANES, across % LANES

    def cols(c):
        return slice(c * extent, (c + 1) * extent)

    def to_right(p, re, im):
        for c, value in ((0, re), (1, im)):
            high, low = split(value)
            right_in[0, cols(p), cols(c)] = high
            right_in[1, cols(p), cols(c)] = low

    def right_stage(index, p):
        for c in range(2):
            part = jnp.dot(right_in[0, cols(p), :], mats[index, 0, :, cols(c)], preferred_element_type=f32)
            part += jnp.dot(right_in[0, cols(p), :], mats[index, 1, :, cols(c)], preferred_element_type=f32)
            part += jnp.dot(right_in[1, cols(p), :], mats[index, 0, :, cols(c)], preferred_element_type=f32)
            high, low = split(part)
            left_in[0, cols(c), cols(p)] = high
            left_in[1, cols(c), cols(p)] = low

    def left_stage(index, p):
        out = []
        for c in range(2):
            part = jnp.dot(mats[index, 0, cols(c), :], left_in[0, :, cols(p)], preferred_element_type=f32)
            part += jnp.dot(mats[index, 1, cols(c), :], left_in[0, :, cols(p)], preferred_element_type=f32)
            part += jnp.dot(mats[index, 0, cols(c), :], left_in[1, :, cols(p)], preferred_element_type=f32)
            out.append(part)
        return out

    def add_piece(p, q, value):
        down, first, turn = place(p)
        moved = [pltpu.roll(value[:, LANES * t : LANES * (t + 1)], turn, 1) for t in range(tiles)]
        for t in range(tiles + 1):
            if t == 0:
                piece = jnp.where(lane >= turn, moved[0], 0.0)
            elif t == tiles:
                piece = jnp.where(lane >= turn, 0.0, moved[t - 1])
            else:
                piece = jnp.where(lane >= turn, moved[t], moved[t - 1])
            grad[q, first + t, pl.ds(down, extent), :] += piece

    def cut(p, planes):
        down, first, turn = place(p)
        back = (LANES - turn) % LANES
        for q in planes:
            got = [pltpu.roll(window[q, first + t, pl.ds(down, extent), :], back, 1) for t in range(tiles + 1)]
            for t in range(tiles):
                patch[p, q, :, LANES * t : LANES * (t + 1)] = jnp.where(lane < LANES - turn, got[t], got[t + 1])

    for p in range(count):
        cut(p, (0, 1))
        pr, pi = probe[0], probe[1]
        ar, ai = patch[p, 0], patch[p, 1]
        to_right(p, pr * ar - pi * ai, pr * ai + pi * ar)
        right_stage(0, p)
    for p in range(count):
        cut(p, (2, 3))
    for p in range(count):
        qr, qi = left_stage(1, p)
        wave[p, 0] = qr
        wave[p, 1] = qi
        br, bi = patch[p, 2], patch[p, 3]
        to_right(p, qr * br - qi * bi, qr * bi + qi * br)
        right_stage(2, p)
    for p in range(count):
        fr, fi = left_stage(3, p)
        excess = 2.0 * (fr * fr + fi * fi - measured[p])
        to_right(p, excess * fr, excess * fi)
        right_stage(3, p)
    for p in range(count):
        hr, hi = left_stage(2, p)
        br, bi = patch[p, 2], patch[p, 3]
        to_right(p, br * hr + bi * hi, br * hi - bi * hr)
        right_stage(1, p)
        qr, qi = wave[p, 0], wave[p, 1]
        add_piece(p, 2, qr * hr + qi * hi)
        add_piece(p, 3, qr * hi - qi * hr)

    def packed(planes, old, tile, left, start, rows):
        narrow = lanes_of(rows)
        for q in planes:
            value = grad[q, tile, pl.ds(start, rows), :]
            turn = (RIM * q + (RIM if left else 0)) % LANES
            value = pltpu.roll(value, turn, 1) if turn else value
            old = value if old is None else jnp.where((narrow >= RIM * q) & (narrow < RIM * (q + 1)), value, old)
        return old

    def emit(planes, begin):
        for ref, tile, left in ((left_out, 0, True), (right_out, tiles + 1, False)):
            ref[...] = packed(planes, None if begin else ref[...], tile, left, RIM, extent)
        for q in planes:
            for t in range(tiles):
                inner_out[q, :, LANES * t : LANES * (t + 1)] = grad[q, t + 1, RIM : RIM + extent, :]
        for n in range(sides):
            base = extent if n == 0 else 0
            for q in planes:
                for t in range(tiles):
                    row_out[n][base + RIM * q : base + RIM * (q + 1), LANES * t : LANES * (t + 1)] = grad[q, t + 1, pl.ds(starts[n], RIM), :]
            at = base + RIM * PLANES
            for tile, left in ((0, True), (tiles + 1, False)):
                where = slice(0, LANES) if left else slice(LANES, 2 * LANES)
                old = None if begin else row_out[n][at : at + RIM, where]
                row_out[n][at : at + RIM, where] = packed(planes, old, tile, left, starts[n], RIM)

    emit((2, 3), True)
    for p in range(count):
        er, ei = left_stage(0, p)
        pr, pi = probe[0], probe[1]
        add_piece(p, 0, pr * er + pi * ei)
        add_piece(p, 1, pr * ei - pi * er)
        ar, ai = patch[p, 0], patch[p, 1]
        gr = ar * er + ai * ei
        gi = ar * ei - ai * er
        if p:
            gr = wave[0, 0] + gr
            gi = wave[0, 1] + gi
        wave[0, 0] = gr
        wave[0, 1] = gi
    is_odd = odd_row == 1
    keep_out[...] = jnp.where(is_odd, wave[0, 1], wave[0, 0])
    row_out[0][:extent, :] = jnp.where(is_odd, wave[0, 0], wave[0, 1])
    emit((0, 1), False)


def corner_kernel(col1, col2, *msgs):
    par = parities()
    extent = col1.shape[0]
    for n, msg in enumerate(msgs):
        start = pl.multiple_of((1 - (par[0] + n) % 2) * (extent - RIM), RIM)
        msg[:RIM, :] = col1[pl.ds(start, RIM), :]
        msg[RIM:, :] = col2[pl.ds(start, RIM), :]


def split_kernel(mine, other, keep, send):
    par = parities()
    half = mine.shape[0] // 2
    kept = pl.multiple_of(par[3] * half, half)
    sent = pl.multiple_of((1 - par[3]) * half, half)
    keep[...] = mine[pl.ds(kept, half), :] + other[pl.ds(kept, half), :]
    send[...] = mine[pl.ds(sent, half), :] + other[pl.ds(sent, half), :]


def cols_kernel(sides, keep, left, right, *rest):
    par = parities()
    row_in = rest[:sides]
    probe_msg, probe_keep, msg1, msg2, edge = rest[sides:]
    extent = left.shape[0]
    half = extent // 2
    odd_col = par[1] == 1
    up = par[2] == 1
    edge[0] = left[...]
    edge[1] = right[...]
    for n in range(sides):
        base = (extent if n == 0 else 0) + RIM * PLANES
        start = pl.multiple_of((1 - (par[0] + n) % 2) * (extent - RIM), RIM)
        for s in range(2):
            edge[s, pl.ds(start, RIM), :] += row_in[n][base : base + RIM, LANES * s : LANES * (s + 1)]
    to1 = jnp.where(odd_col, edge[0], edge[1])
    to2 = jnp.where(odd_col, edge[1], edge[0])
    lower = keep[:half, :] + row_in[0][:half, :]
    upper = keep[half:, :] + row_in[0][half:extent, :]
    probe_keep[...] = jnp.where(up, upper, lower)
    probe_msg[...] = jnp.where(up, lower, upper)
    for msg, value in ((msg1, to1), (msg2, to2)):
        msg[:, :LANES] = value[:half]
        msg[:, LANES:] = value[half:]


def gather_kernel(sides, inner, keep3, got3, col1, col2, *rest):
    row_in = rest[:sides]
    msg, descent = rest[sides:]
    par = parities()
    extent = inner.shape[-1]
    half = extent // 2
    quarter = keep3.shape[0]
    odd_col = par[1] == 1
    lane = lanes_of(half)
    descent[...] = inner[...]
    for n in range(sides):
        base = extent if n == 0 else 0
        start = pl.multiple_of((1 - (par[0] + n) % 2) * (extent - RIM), RIM)
        for q in range(PLANES):
            descent[q, pl.ds(start, RIM), :] += row_in[n][base + RIM * q : base + RIM * (q + 1), :]
    for s in range(2):
        rim1 = col1[:, LANES * s : LANES * (s + 1)]
        rim2 = col2[:, LANES * s : LANES * (s + 1)]
        from_left = jnp.where(odd_col, rim1, rim2)
        from_right = jnp.where(odd_col, rim2, rim1)
        rows = slice(half * s, half * (s + 1))
        for q in range(PLANES):
            turn_left = (LANES - RIM * q) % LANES
            turn_right = (LANES - RIM - RIM * q) % LANES
            on_left = pltpu.roll(from_left, turn_left, 1) if turn_left else from_left
            on_right = pltpu.roll(from_right, turn_right, 1) if turn_right else from_right
            descent[q, rows, :LANES] += jnp.where(lane < RIM, on_left, 0.0)
            descent[q, rows, extent - LANES :] += jnp.where(lane >= LANES - RIM, on_right, 0.0)
    peak = None
    for s in range(2):
        power = descent[2 * s] * descent[2 * s] + descent[2 * s + 1] * descent[2 * s + 1]
        power = jnp.max(power.reshape(extent // 8, 8, extent), axis=0)
        peak = power if peak is None else jnp.maximum(peak, power)
    msg[:quarter, :] = keep3[...] + got3[...]
    msg[quarter:, :] = peak


def final_kernel(rate, obj, descent, probe, mine, other, obj_out, probe_out, buf, sem):
    extent = obj.shape[-1]
    odd_row = parities()[0] == 1
    sums = (jnp.where(odd_row, other[:extent, :], mine[:extent, :]), jnp.where(odd_row, mine[:extent, :], other[:extent, :]))
    copies = [pltpu.make_async_copy(buf.at[q], obj_out.at[q], sem.at[q]) for q in range(PLANES)]
    copies += [pltpu.make_async_copy(buf.at[PLANES + c], probe_out.at[c], sem.at[PLANES + c]) for c in range(2)]
    for c in range(2):
        buf[PLANES + c] = probe[c] - rate * sums[c]
        copies[PLANES + c].start()
    peak = jnp.max(jnp.maximum(mine[extent:, :], other[extent:, :]))
    peak = jnp.broadcast_to(peak, (8, extent))
    scale = (0.3 / (jnp.sqrt(peak) + 1e-06))[:1, :]
    for q in range(PLANES):
        buf[q] = obj[q] - descent[q] * scale
        copies[q].start()
    for copy in copies:
        copy.wait()


def call(kernel, outs, ins, scratch=(), in_hbm=(), out_hbm=(), alias=None, limit=8):
    shapes = [out if isinstance(out, jax.ShapeDtypeStruct) else jax.ShapeDtypeStruct(out, f32) for out in outs]
    return pl.pallas_call(
        kernel,
        out_shape=tuple(shapes),
        in_specs=[HBM if i in in_hbm else VMEM for i in range(len(ins))],
        out_specs=tuple(HBM if i in out_hbm else VMEM for i in range(len(outs))),
        scratch_shapes=list(scratch),
        input_output_aliases=alias or {},
        compiler_params=pltpu.CompilerParams(vmem_limit_bytes=limit * 1024 * 1024),
    )(*[pltpu.with_memory_space_constraint(x, pltpu.HBM) if i in in_hbm else x for i, x in enumerate(ins)])


def swap(value, axis, bit):
    count = lax.axis_size(axis)
    return lax.ppermute(value, axis, [(i, i ^ bit) for i in range(count)])


def pairs(value, axis, phase):
    count = lax.axis_size(axis)
    links = []
    for i in range(phase, count - 1, 2):
        links += [(i, i + 1), (i + 1, i)]
    return lax.ppermute(value, axis, links)


def step(object_in, probe_in, positions, intensity):
    extent = probe_in.shape[-1]
    half, quarter = extent // 2, extent // 4
    rows, cols = lax.axis_size("row"), lax.axis_size("col")
    sides = 1 if rows == 2 else 2
    count = positions.size // 2
    measured_in = intensity.reshape(-1, extent, extent)
    obj_in = object_in.reshape(PLANES, extent, extent)
    tabs = jnp.asarray(tables(extent))
    span = extent + 2 * RIM
    tiles = extent // LANES
    rim_rows = RIM * (PLANES + 1)

    obj, *sent = call(
        pack_kernel,
        [obj_in.shape] + [(extent, LANES)] * 2 + [(PLANES * RIM, extent)] * sides,
        (obj_in,),
        scratch=[pltpu.SemaphoreType.DMA((PLANES,))],
        in_hbm=(0,),
    )
    col2 = pairs(sent[1], "col", 1)
    col1 = pairs(sent[0], "col", 0)
    row_in = [pairs(sent[2 + n], "row", n) for n in range(sides)]
    probe, measured, mats, window, grad, mask2, mask4, offsets = call(
        prep_kernel,
        [
            probe_in.shape,
            measured_in.shape,
            jax.ShapeDtypeStruct((4, 2, 2 * extent, 2 * extent), bf16),
            (PLANES, tiles + 2, span, LANES),
            (PLANES, tiles + 2, span, LANES),
            (half, extent),
            (quarter, extent),
            jax.ShapeDtypeStruct((count, 2), jnp.int32),
        ],
        (obj, probe_in, measured_in, tabs, positions.reshape(-1, 2)),
        scratch=[pltpu.VMEM(tabs.shape, bf16), pltpu.SemaphoreType.DMA((4,))],
        in_hbm=(1, 2, 3, 4),
        limit=16,
    )
    corners = call(corner_kernel, [(2 * RIM, LANES)] * sides, (col1, col2))
    corner_in = [pairs(corners[n], "row", n) for n in range(sides)]

    ins = (offsets, col1, col2, *row_in, *corner_in, probe, measured, mats, window, grad)
    shapes = [(extent + rim_rows, extent)] + [(rim_rows, extent)] * (sides - 1)
    shapes += [(extent, extent), (PLANES, extent, extent), (extent, LANES), (extent, LANES), window.shape, grad.shape]
    out = call(
        functools.partial(tile_kernel, sides),
        shapes,
        ins,
        scratch=[
            pltpu.VMEM((count, PLANES, extent, extent), f32),
            pltpu.VMEM((count, 2, extent, extent), f32),
            pltpu.VMEM((2, count * extent, 2 * extent), bf16),
            pltpu.VMEM((2, 2 * extent, count * extent), bf16),
            pltpu.SMEM(offsets.shape, jnp.int32),
            pltpu.SemaphoreType.DMA,
        ],
        alias={len(ins) - 2: len(shapes) - 2, len(ins) - 1: len(shapes) - 1},
        limit=32,
    )
    row_back = [pairs(out[n], "row", n) for n in range(sides)]
    keep, inner, left, right = out[sides : sides + 4]
    probe_msg, probe_keep, msg1, msg2 = call(
        functools.partial(cols_kernel, sides),
        [(half, extent)] * 4,
        (keep, left, right, *row_back),
        scratch=[pltpu.VMEM((2, extent, LANES), f32)],
    )
    probe_got = swap(probe_msg, "col", 2)
    got2 = pairs(msg2, "col", 1)
    got1 = pairs(msg1, "col", 0)
    keep3, send3 = call(split_kernel, [(quarter, extent)] * 2, (probe_keep, probe_got))
    got3 = swap(send3, "col", 4)
    state, descent = call(
        functools.partial(gather_kernel, sides),
        [(quarter + 8, extent), (PLANES, extent, extent)],
        (inner, keep3, got3, got1, got2, *row_back),
    )
    is_sum = lax.broadcasted_iota(jnp.int32, state.shape, 0) < quarter
    steps = [("col", 1 << b) for b in range(3, cols.bit_length() - 1)] + [("col", 1)]
    steps += [("row", 1 << b) for b in range(1, rows.bit_length() - 1)]
    for axis, bit in steps:
        other = swap(state, axis, bit)
        state = jnp.where(is_sum, state + other, jnp.maximum(state, other))

    def joined(state, other, mask):
        top = state.shape[0] - 8
        up = mask > 0.5
        low = jnp.where(up, other[:top], state[:top])
        high = jnp.where(up, state[:top], other[:top])
        return jnp.concatenate([low, high, jnp.maximum(state[top:], other[top:])], 0)

    state = joined(state, swap(state, "col", 4), mask4)
    state = joined(state, swap(state, "col", 2), mask2)
    other = swap(state, "row", 1)
    object_out, probe_out = call(
        functools.partial(final_kernel, 2.0 / (rows * cols)),
        [obj.shape, probe_in.shape],
        (obj, descent, probe, state, other),
        scratch=[pltpu.VMEM((PLANES + 2, extent, extent), f32), pltpu.SemaphoreType.DMA((PLANES + 2,))],
        out_hbm=(0, 1),
    )
    return object_out.reshape(object_in.shape), probe_out


def solution(mesh):
    placed = (
        P(None, None, "row", "col"),
        P(),
        P("row", "col", None, None),
        P("row", "col", None, None, None),
    )
    return jax.shard_map(
        step,
        mesh=mesh,
        in_specs=placed,
        out_specs=(P(None, None, "row", "col"), P()),
        check_vma=False,
    )
```
